32 devices in a mesh: cls: 4 (over y, x), dom: 8 (over z, core).
Axes of the slice: x: 2, y: 2, z: 4, core: 2. Of those that a mesh axis runs over, the one named last changes fastest.
Arguments:
- particles: bfloat16 [256, 2, 110592], P(('cls', 'dom')), may hold values from -18 to 18
- labels: int32 [256, 1], P(('cls', 'dom')), may hold values from 0 to 7; in each aligned block of 8 rows (0 to 7, 8 to 15, ...) at most 2 rows name the same one
- wedge_index: int32 [256], P(('cls', 'dom')), may hold values from 0 to 11
- wedge_table: float32 [12, 110592], replicated, may hold values from 0.05 to 1
Outputs:
- class_average: float32 [8, 2, 110592], P('cls', None, 'dom')
- weight_total: float32 [8, 110592], P('cls', 'dom')
The draws below stay inside these ranges and needn't reach their ends.
Inputs may be any that keep to these rules, and one draw needn't show every extreme that they name: `labels`: among the rows of one device no class appears more than 2 times, and on some devices one class appears exactly 2 times; every class appears on some device.
All inputs are finite; a program needn't handle non-finite values.
Results may differ from the reference program's by a relative error of at most 0.0003.
Values may be sent and summed in bfloat16 or wider, within the bound.
A program may use at most 128 MiB of HBM per device.

```python
import math
import jax
import jax.numpy as jnp
import numpy as np
from jax import lax

P_DEV = 8
WEDGES = 12
CLASSES = 8
MOST = 2
VOX = 110592
PARTICLES = 256


def place_ends(values, stream_key, least, top_value):
    dims = values.shape
    index_at = [jax.random.randint(jax.random.fold_in(stream_key, axis), (), 0, dims[axis]) for axis in range(len(dims))]
    values = values.at[tuple(index_at)].set(least)
    longest = dims.index(max(dims))
    index_at[longest] = (index_at[longest] + 1) % dims[longest]
    return values.at[tuple(index_at)].set(top_value)


def level_of(key, shape, pieces, least, high):
    level = 1.0
    for position, parts in pieces:
        draws = jax.random.uniform(jax.random.fold_in(jax.random.fold_in(key, 6), position), (parts,), jnp.float32, least / len(pieces), high / len(pieces))
        level = level * jnp.repeat(jnp.exp(draws), shape[position] // parts).reshape((-1,) + (1,) * (len(shape) - 1 - position))
    return level


def shared_out(own_key, own, number, rows, count, top, limit, slope):
    ranking = jax.random.permutation(own_key, count)
    heavy_load, ordinary = shares(count, rows * top, limit, slope, True), shares(count, rows * top, limit, slope, False)
    places = jnp.arange(count)

    def named(tallies, turn):
        used = int((tallies > 0).sum())
        fixed = max(1, used // 4)
        shifted = fixed + (places - fixed + turn * (used - fixed)) % max(1, count - fixed)
        return jnp.zeros((count,), jnp.int32).at[ranking[jnp.where(places < fixed, places, shifted)]].set(jnp.asarray(tallies, jnp.int32))

    tallies = jnp.where(number % 4 == 0, named(heavy_load, number // 4), named(ordinary, number - number // 4 - 1))
    mixed = jax.random.permutation(jax.random.fold_in(own, 3), count)
    donor, taker = mixed[0:count // 2 * 2:2], mixed[1:count // 2 * 2:2]
    slack = jnp.minimum(tallies[donor] - 1, limit - tallies[taker]) // 2
    slack = jnp.where((donor == ranking[0]) | (taker == ranking[0]) | (tallies[taker] == 0), 0, jnp.maximum(slack, 0))
    shifted = jax.random.randint(jax.random.fold_in(own, 4), (count // 2,), 0, 1 << 20) % (slack + 1)
    tallies = tallies.at[donor].add(-shifted).at[taker].add(shifted)
    items = jnp.searchsorted(jnp.cumsum(tallies), jnp.arange(rows * top), side="right").astype(jnp.int32)
    grid = items.reshape(top, rows).T
    grid = grid[jax.random.permutation(jax.random.fold_in(own, 1), rows)]
    turn = jax.random.randint(jax.random.fold_in(own, 2), (rows, 1), 0, top)
    return jnp.take_along_axis(grid, (jnp.arange(top)[None, :] + turn) % top, axis=1)


def shares(number_of, total, bound, skew, full):
    loads = [(1 << 20) // math.isqrt(standing ** skew) + 1 for standing in range(1, number_of + 1)]
    largest = bound if full else min(bound, max(-(-total // number_of), total * loads[0] // sum(loads)))
    least = 1 if total - largest >= number_of - 1 else 0
    holding, surplus = [largest] + [least] * (number_of - 1), total - largest - least * (number_of - 1)
    while surplus > 0:
        free = [i for i in range(1, number_of) if holding[i] < largest] or [i for i in range(1, number_of) if holding[i] < bound]
        mass, remaining = sum([loads[i] for i in free]), surplus
        for i in free:
            extra = min(bound - holding[i], max(1, remaining * loads[i] // mass), surplus)
            holding[i] = holding[i] + extra
            surplus = surplus - extra
    return np.array(holding)


def bell_draw(rng, shape, spread, limit, split=(), kind=jnp.bfloat16):
    array = spread * jax.random.normal(rng, shape, jnp.float32)
    if split:
        array = array * level_of(rng, shape, split, -0.22, 0.18)
    return jnp.clip(array, -limit, limit).astype(kind)


def setup_inputs(seed: int = 0) -> dict:
    keys = jax.random.split(jax.random.key(seed), 5)
    particles = bell_draw(keys[0], (PARTICLES, 2, VOX), 3.0, 18.0, ((0, 32),))
    labels_keys = jax.random.split(jax.random.fold_in(keys[1], 1), PARTICLES // P_DEV)
    labels_turns = jax.random.permutation(jax.random.fold_in(keys[1], 3), PARTICLES // P_DEV)
    labels = jax.vmap(lambda own, number: shared_out(jax.random.fold_in(keys[1], 2), own, number, P_DEV, CLASSES, 1, MOST, 2))(labels_keys, labels_turns).reshape((PARTICLES, 1))
    wedge_index = place_ends(jax.random.randint(keys[2], (PARTICLES,), 0, WEDGES), jax.random.fold_in(keys[2], 1), 0, WEDGES - 1).astype(jnp.int32)
    wedge_table = jnp.clip(jnp.exp(jax.random.uniform(keys[3], (WEDGES, VOX), jnp.float32, math.log(0.05), math.log(1.0))), 0.05, 1.0)
    return {"particles": particles, "labels": labels, "wedge_index": wedge_index, "wedge_table": wedge_table}


def reference(particles, labels, wedge_index, wedge_table):
    count = particles.shape[0]
    block = 64 if count % 64 == 0 else count
    steps_total = count // block
    classes_all = CLASSES
    label_flat = labels[:, 0]

    def accumulate(carry, index):
        start = (index * block).astype(jnp.int32)
        piece = lax.dynamic_slice_in_dim(particles, start, block, 0).astype(jnp.float32)
        label_piece = lax.dynamic_slice_in_dim(label_flat, start, block, 0)
        wedge_piece = lax.dynamic_slice_in_dim(wedge_index, start, block, 0)
        pick = (wedge_piece[:, None] == jnp.arange(WEDGES, dtype=jnp.int32)[None, :]).astype(jnp.float32)
        weight = jnp.dot(pick, wedge_table, precision=lax.Precision.HIGHEST)
        member = (jnp.arange(classes_all, dtype=jnp.int32)[:, None] == label_piece[None, :]).astype(jnp.float32)
        numer = jnp.einsum("kb,bcv->kcv", member, weight[:, None, :] * piece, precision=lax.Precision.HIGHEST)
        denom = jnp.dot(member, weight * weight, precision=lax.Precision.HIGHEST)
        return (carry[0] + numer, carry[1] + denom), None

    start_sums = (jnp.zeros((classes_all, 2, VOX), jnp.float32), jnp.zeros((classes_all, VOX), jnp.float32))
    (weighted_sum, weight_total), unused = lax.scan(accumulate, start_sums, jnp.arange(steps_total, dtype=jnp.int32))
    class_average = weighted_sum / (weight_total[:, None, :] + 1.0)
    return class_average, weight_total
```

```python
import functools

import jax
import jax.numpy as jnp
from jax import lax
from jax.experimental import pallas as pl
from jax.experimental.pallas import tpu as pltpu
from jax.sharding import PartitionSpec as P

MESH = pl.DeviceIdType.MESH
LANES = 128
LEVELS = 32767.0
CLASSES_PER_GROUP = 2
GROUP_ROWS = 2 * CLASSES_PER_GROUP
PAIR_ROWS = 2 * GROUP_ROWS
PICK_TILES = 36
SUM_TILES = 27
CODE_TILES = 27
FORWARD_LAG = 2
SETTLE_LAG = 4


def divisor(number, cap):
    return max(size for size in range(1, cap + 1) if number % size == 0)


def dot(left, right):
    return jnp.dot(left, right, preferred_element_type=jnp.float32)


def stack2(value):
    high = value.astype(jnp.bfloat16)
    low = (value - high.astype(jnp.float32)).astype(jnp.bfloat16)
    return jnp.concatenate([high, low], axis=0)


def stack2_rows(value):
    high = value.astype(jnp.bfloat16).astype(jnp.float32)
    return jnp.concatenate([high, value - high], axis=0).astype(jnp.bfloat16)


def walk(start, tiles, cap, body):
    unit = divisor(tiles, cap)
    turns = tiles // unit
    if turns == 1:
        body(pl.ds(start, unit * LANES), unit)
        return

    @pl.loop(0, turns)
    def _(index):
        body(pl.ds(pl.multiple_of(start + index * (unit * LANES), LANES), unit * LANES), unit)


def wide(value, unit):
    return jnp.concatenate([value] * unit, axis=1) if unit > 1 else value


def to_code(value):
    return jnp.round(value).astype(jnp.int32).astype(jnp.int16)


def from_code(code):
    return code.astype(jnp.int32).astype(jnp.float32)


def plan_units(n_z, tiles):
    half = tiles // 2
    plain = ((0, half, 0), (half, tiles - half, 1))
    units = []
    for step in range(n_z):
        for part, (start, count, kind) in enumerate(plain):
            units.append((step, part, start * LANES, count, kind))
    return units


def kernel(
    n_z, shard, p_dev, wedges, units,
    labels_ref, wedge_ref, x_ref, table_ref, mean_ref, total_ref,
    label_s, wedge_s, aux_own, aux_peer, x_all, table, weights, sums, inverse, tops,
    q1, r1, c1, d1, q2, r2, c2, d2, q3, r3, c3, d3,
    t1, u1, t2, u2, t3, u3,
    small_sem, load_sem, table_sem, pair_send, pair_recv, aux_send, aux_recv,
    s1, g1, s2, g2, s3, g3, ts, tg,
):
    cls = lax.axis_index("cls")
    dom = lax.axis_index("dom")
    z = dom // 2
    core = lax.rem(dom, 2)
    peer = dom + 1 - 2 * core
    near = cls + 1 - 2 * lax.rem(cls, 2)
    far = cls + 2 - 4 * (cls // 2)
    both = near + 2 - 4 * (cls // 2)
    rows = 2 * p_dev
    tiles = shard // LANES
    last = n_z - 1
    offsets = sorted(range(1, n_z), key=lambda gap: -min(gap, n_z - gap)) + [0]

    def place(step):
        return lax.rem(z + offsets[step], n_z)

    small = [
        pltpu.make_async_copy(labels_ref, label_s, small_sem.at[0]),
        pltpu.make_async_copy(wedge_ref, wedge_s, small_sem.at[1]),
    ]
    for copy in small:
        copy.start()

    barrier = pltpu.get_barrier_semaphore()
    pl.semaphore_signal(barrier, inc=1, device_id={"dom": peer}, device_id_type=MESH)
    pl.semaphore_signal(barrier, inc=1, device_id={"cls": near}, device_id_type=MESH)
    pl.semaphore_signal(barrier, inc=1, device_id={"cls": far}, device_id_type=MESH)
    for step in range(last):
        pl.semaphore_signal(
            barrier, inc=1, device_id={"dom": place(step) * 2 + core}, device_id_type=MESH
        )

    loads, tables = [], []
    for step in range(n_z):
        here = place(step) * 2 + core
        span = pl.ds(pl.multiple_of(here * shard, LANES), shard)
        copy = pltpu.make_async_copy(table_ref.at[:, span], table.at[step], table_sem.at[step])
        copy.start()
        tables.append(copy)
        copies = []
        for p in range(p_dev):
            copy = pltpu.make_async_copy(
                x_ref.at[p, :, span], x_all.at[step, pl.ds(2 * p, 2)], load_sem.at[step, p]
            )
            copy.start()
            copies.append(copy)
        loads.append(copies)

    for copy in small:
        copy.wait()
    row = lax.broadcasted_iota(jnp.int32, (rows, LANES), 0)
    lane = lax.broadcasted_iota(jnp.int32, (rows, LANES), 1)
    out_row = lax.broadcasted_iota(jnp.int32, (4 * GROUP_ROWS, LANES), 0)
    out_lane = lax.broadcasted_iota(jnp.int32, (4 * GROUP_ROWS, LANES), 1)
    wedge_of = jnp.zeros((rows, LANES), jnp.int32)
    label_of = jnp.zeros_like(out_row)
    particle = (out_lane & (rows - 1)) // 2
    for p in range(p_dev):
        wedge_of = jnp.where(row // 2 == p, wedge_s[p], wedge_of)
        label_of = jnp.where(particle == p, label_s[p], label_of)
    column = jnp.where(lane >= wedges, lane - wedges, lane)
    aux_own[0] = ((wedge_of == column) & (lane < 2 * wedges)).astype(jnp.float32)
    within = (out_row // 2) % CLASSES_PER_GROUP
    place_of = out_row // GROUP_ROWS
    for kind, order in enumerate(((cls, far, near, both), (cls, near, far, both))):
        target = jnp.zeros_like(out_row)
        for slot, group in enumerate(order):
            target = jnp.where(place_of == slot, CLASSES_PER_GROUP * group + within, target)
        aux_own[1 + kind] = (
            (target == label_of) & ((out_row & 1) == (out_lane & 1))
        ).astype(jnp.float32)

    pl.semaphore_wait(barrier, n_z + 2)

    aux_copy = pltpu.make_async_remote_copy(
        src_ref=aux_own, dst_ref=aux_peer, send_sem=aux_send, recv_sem=aux_recv,
        device_id={"dom": peer}, device_id_type=MESH,
    )
    aux_copy.start()
    pair = []
    for step in range(n_z):
        there = place(step) * 2 + (1 - core)
        span = pl.ds(pl.multiple_of(there * shard, LANES), shard)
        copies = []
        for p in range(p_dev):
            copy = pltpu.make_async_remote_copy(
                src_ref=x_ref.at[p, :, span], dst_ref=x_all.at[step, pl.ds(rows + 2 * p, 2)],
                send_sem=pair_send.at[step, p], recv_sem=pair_recv.at[step, p],
                device_id={"dom": peer}, device_id_type=MESH,
            )
            copy.start()
            copies.append(copy)
        pair.append(copies)
    aux_copy.wait()

    own_side = (out_lane & rows) == 0
    members = [
        jnp.where(own_side, aux_own[1 + kind], aux_peer[1 + kind])[:, : 4 * rows].astype(jnp.bfloat16)
        for kind in range(2)
    ]
    pick = jnp.concatenate([aux_own[0], aux_peer[0]], axis=0).astype(jnp.bfloat16)
    counts = dot(members[0][:, : 2 * rows], pick)
    pick = pick[:, : 2 * wedges]

    def send(source, target, sems, who):
        copy = pltpu.make_async_remote_copy(
            src_ref=source, dst_ref=target, send_sem=sems[0], recv_sem=sems[1],
            device_id=who, device_id_type=MESH,
        )
        copy.start()
        return copy

    t1[...] = counts[PAIR_ROWS:]
    tally_copies = [send(t1, u1, (ts.at[0], tg.at[0]), {"cls": near})]

    for step in range(n_z):
        tables[step].wait()

        def pick_body(span, unit):
            weights[step, :, span] = dot(pick, stack2_rows(table[step, :, span]))

        walk(0, tiles, PICK_TILES, pick_body)

    first, second, third = {}, {}, {}

    def compute(index):
        step, part, start, count, kind = units[index]
        if start == 0:
            for copy in loads[step] + pair[step]:
                copy.wait()
        member = members[kind]
        tops[index] = jnp.zeros((4 * GROUP_ROWS, LANES), jnp.float32)

        def body(span, unit):
            product = weights[step, :, span] * x_all[step, :, span].astype(jnp.float32)
            total = dot(member, stack2(product))
            sums[step, :, span] = total
            size = jnp.abs(total)
            pieces = [size[:, k * LANES : (k + 1) * LANES] for k in range(unit)]
            while len(pieces) > 1:
                pieces = [
                    jnp.maximum(*pieces[k : k + 2]) if k + 1 < len(pieces) else pieces[k]
                    for k in range(0, len(pieces), 2)
                ]
            tops[index] = jnp.maximum(tops[index], pieces[0])

        walk(start, count, SUM_TILES, body)
        top = jnp.maximum(tops[index, pl.ds(PAIR_ROWS, PAIR_ROWS)], 1e-30)
        c1[index] = top
        factor = LEVELS / top

        def code_body(span, unit):
            q1[step, :, span] = to_code(
                sums[step, pl.ds(PAIR_ROWS, PAIR_ROWS), span] * wide(factor, unit)
            )

        walk(start, count, CODE_TILES, code_body)
        partner = near if kind == 0 else far
        span = pl.ds(start, count * LANES)
        first[index] = [
            send(c1.at[index], d1.at[index], (s1.at[index, 0], g1.at[index, 0]), {"cls": partner}),
            send(q1.at[step, :, span], r1.at[step, :, span], (s1.at[index, 1], g1.at[index, 1]), {"cls": partner}),
        ]

    def forward(index):
        step, part, start, count, kind = units[index]
        for copy in first[index]:
            copy.wait()
        got = d1[index]
        bound = jnp.maximum(tops[index, pl.ds(0, PAIR_ROWS)], 1e-30) + got
        tops[index, pl.ds(0, PAIR_ROWS)] = bound
        scale = got * (1.0 / LEVELS)
        factor = LEVELS / bound
        c2[index] = bound[GROUP_ROWS:]

        def body(span, unit):
            total = sums[step, pl.ds(0, PAIR_ROWS), span] + from_code(r1[step, :, span]) * wide(scale, unit)
            sums[step, pl.ds(0, PAIR_ROWS), span] = total
            q2[step, :, span] = to_code(total * wide(factor, unit))[GROUP_ROWS:]

        walk(start, count, CODE_TILES, body)
        other = far if kind == 0 else near
        span = pl.ds(start, count * LANES)
        second[index] = [
            send(c2.at[index], d2.at[index], (s2.at[index, 0], g2.at[index, 0]), {"cls": other}),
            send(q2.at[step, :, span], r2.at[step, :, span], (s2.at[index, 1], g2.at[index, 1]), {"cls": other}),
        ]

    def settle(index):
        step, part, start, count, kind = units[index]
        for copy in second[index]:
            copy.wait()
        got = d2[index]
        scale = got * (1.0 / LEVELS)
        if step == last:

            def final_body(span, unit):
                value = sums[step, pl.ds(0, GROUP_ROWS), span] + from_code(r2[step, :, span]) * wide(scale, unit)
                mean_ref[:, span] = value * inverse[:, span]

            walk(start, count, CODE_TILES, final_body)
            return
        bound = tops[index, pl.ds(0, GROUP_ROWS)] + got
        c3[index] = bound
        factor = LEVELS / bound

        def body(span, unit):
            value = sums[step, pl.ds(0, GROUP_ROWS), span] + from_code(r2[step, :, span]) * wide(scale, unit)
            q3[step, :, span] = to_code(value * wide(factor, unit))

        walk(start, count, CODE_TILES, body)
        there = {"dom": place(step) * 2 + core}
        span = pl.ds(start, count * LANES)
        third[index] = [
            send(c3.at[index], d3.at[index], (s3.at[index, 0], g3.at[index, 0]), there),
            send(q3.at[step, :, span], r3.at[step, :, span], (s3.at[index, 1], g3.at[index, 1]), there),
        ]

    def gather(index):
        step, part, start, count, kind = units[index]
        mine = [k for k, unit in enumerate(units) if unit[0] < last and unit[1] == part]
        for k in mine:
            for copy in third[k]:
                copy.wait()
        scales = [d3[k] * (1.0 / LEVELS) for k in mine]

        def body(span, unit):
            value = sums[step, pl.ds(0, GROUP_ROWS), span]
            for k, scale in zip(mine, scales):
                value = value + from_code(r3[units[k][0], :, span]) * wide(scale, unit)
            sums[step, pl.ds(0, GROUP_ROWS), span] = value

        walk(start, count, CODE_TILES, body)

    def tally_forward():
        tally_copies[0].wait()
        gathered = counts[:PAIR_ROWS] + u1[...]
        t2[...] = gathered
        tally_copies.append(send(t2, u2, (ts.at[1], tg.at[1]), {"cls": far}))

    def tally_settle():
        tally_copies[1].wait()
        t3[...] = t2[pl.ds(0, GROUP_ROWS)] + u2[pl.ds(GROUP_ROWS, GROUP_ROWS)]
        for step in range(last):
            tally_copies.append(
                send(t3, u3.at[step], (ts.at[2 + step], tg.at[2 + step]), {"dom": place(step) * 2 + core})
            )

    def tally_final():
        tally = t3[...]
        for step in range(last):
            tally_copies[2 + step].wait()
            tally = tally + u3[step]
        tally = stack2_rows(tally[:, : 2 * wedges])

        def body(span, unit):
            weight = table[last, :, span]
            total = dot(tally, stack2_rows(weight * weight))
            total = total[:GROUP_ROWS] + total[GROUP_ROWS:]
            total_ref[:, span] = total
            inverse[:, span] = 1.0 / (total + 1.0)

        walk(0, tiles, SUM_TILES, body)

    n_units = len(units)
    for turn in range(n_units):
        compute(turn)
        if turn == 1:
            tally_forward()
        if turn == 3:
            tally_settle()
        if turn == 5:
            tally_final()
        if turn >= FORWARD_LAG:
            forward(turn - FORWARD_LAG)
        if turn >= SETTLE_LAG:
            settle(turn - SETTLE_LAG)
    lasts = [k for k, unit in enumerate(units) if unit[0] == last]
    pending = [k for k in range(max(0, n_units - SETTLE_LAG), n_units)]
    for k in range(max(0, n_units - FORWARD_LAG), n_units):
        forward(k)
        if pending and pending[0] not in lasts:
            settle(pending.pop(0))
    while pending and pending[0] not in lasts:
        settle(pending.pop(0))
    for k in lasts:
        gather(k)
    for k in pending:
        settle(k)


def finish(mean_ref, total_ref, avg_out, total_out):
    for index in range(avg_out.shape[0]):
        avg_out[index] = mean_ref[pl.ds(2 * index, 2)]
        total_out[pl.ds(index, 1)] = total_ref[pl.ds(2 * index, 1)]


def per_device(particles, labels, wedge_index, wedge_table):
    n_dom = lax.axis_size("dom")
    p_dev, _, voxels = particles.shape
    wedges = wedge_table.shape[0]
    shard = voxels // n_dom
    n_z = n_dom // 2
    rows = 2 * p_dev
    tiles = shard // LANES
    units = plan_units(n_z, tiles)
    count = len(units)
    any_space = pl.BlockSpec(memory_space=pl.ANY)
    vmem = pl.BlockSpec(memory_space=pltpu.VMEM)
    dma = pltpu.SemaphoreType.DMA
    f32 = jnp.float32
    scratch = [
        pltpu.SMEM((p_dev,), jnp.int32),
        pltpu.SMEM((p_dev,), jnp.int32),
        pltpu.VMEM((3, rows, LANES), f32),
        pltpu.VMEM((3, rows, LANES), f32),
        pltpu.VMEM((n_z, 2 * rows, shard), jnp.bfloat16),
        pltpu.VMEM((n_z, wedges, shard), f32),
        pltpu.VMEM((n_z, 2 * rows, shard), f32),
        pltpu.VMEM((n_z, 4 * GROUP_ROWS, shard), f32),
        pltpu.VMEM((GROUP_ROWS, shard), f32),
        pltpu.VMEM((count, 4 * GROUP_ROWS, LANES), f32),
    ]
    for height in (PAIR_ROWS, GROUP_ROWS, GROUP_ROWS):
        scratch += [pltpu.VMEM((n_z, height, shard), jnp.int16)] * 2
        scratch += [pltpu.VMEM((count, height, LANES), f32)] * 2
    scratch += [pltpu.VMEM((PAIR_ROWS, LANES), f32)] * 4
    scratch += [pltpu.VMEM((GROUP_ROWS, LANES), f32), pltpu.VMEM((n_z, GROUP_ROWS, LANES), f32)]
    scratch += [dma((2,)), dma((n_z, p_dev)), dma((n_z,)), dma((n_z, p_dev)), dma((n_z, p_dev)), dma, dma]
    scratch += [dma((count, 2))] * 6
    scratch += [dma((n_z + 1,))] * 2
    mean, total = pl.pallas_call(
        functools.partial(kernel, n_z, shard, p_dev, wedges, units),
        out_shape=(
            jax.ShapeDtypeStruct((GROUP_ROWS, shard), f32),
            jax.ShapeDtypeStruct((GROUP_ROWS, shard), f32),
        ),
        in_specs=[any_space] * 4,
        out_specs=(vmem, vmem),
        scratch_shapes=scratch,
        compiler_params=pltpu.CompilerParams(
            collective_id=0, has_side_effects=True, vmem_limit_bytes=48 * 1024 * 1024
        ),
    )(labels.reshape(p_dev), wedge_index, particles, wedge_table)
    return pl.pallas_call(
        finish,
        out_shape=(
            jax.ShapeDtypeStruct((CLASSES_PER_GROUP, 2, shard), f32),
            jax.ShapeDtypeStruct((CLASSES_PER_GROUP, shard), f32),
        ),
        in_specs=[vmem, vmem],
        out_specs=(vmem, vmem),
    )(mean, total)


def solution(mesh):
    return jax.shard_map(
        per_device,
        mesh=mesh,
        in_specs=(P(("cls", "dom"), None, None), P(("cls", "dom"), None), P(("cls", "dom")), P()),
        out_specs=(P("cls", None, "dom"), P("cls", "dom")),
        check_vma=False,
    )
```

```python
import functools

import jax
import jax.numpy as jnp
from jax import lax
from jax.experimental import pallas as pl
from jax.experimental.pallas import tpu as pltpu
from jax.sharding import PartitionSpec as P

MESH = pl.DeviceIdType.MESH
LANES = 128
LEVELS = 32767.0
SCALE_STEPS = 128.0
TINY = 1e-30
HEAD = 2
CLASSES_PER_GROUP = 2
GROUP_ROWS = 2 * CLASSES_PER_GROUP
PAIR_ROWS = 2 * GROUP_ROWS
PICK_TILES = 36
SUM_TILES = 27
CODE_TILES = 27
FORWARD_LAG = 2
SETTLE_LAG = 4


def divisor(number, cap):
    return max(size for size in range(1, cap + 1) if number % size == 0)


def dot(left, right):
    return jnp.dot(left, right, preferred_element_type=jnp.float32)


def stack2(value):
    high = value.astype(jnp.bfloat16)
    low = (value - high.astype(jnp.float32)).astype(jnp.bfloat16)
    return jnp.concatenate([high, low], axis=0)


def stack2_rows(value):
    high = value.astype(jnp.bfloat16).astype(jnp.float32)
    return jnp.concatenate([high, value - high], axis=0).astype(jnp.bfloat16)


def walk(start, tiles, cap, body):
    unit = divisor(tiles, cap)
    turns = tiles // unit
    if turns == 1:
        body(pl.ds(start, unit * LANES), unit)
        return

    @pl.loop(0, turns)
    def _(index):
        body(pl.ds(pl.multiple_of(start + index * (unit * LANES), LANES), unit * LANES), unit)


def wide(value, unit):
    return jnp.concatenate([value] * unit, axis=1) if unit > 1 else value


def to_code(value):
    return jnp.round(value).astype(jnp.int32).astype(jnp.int16)


def from_code(code):
    return code.astype(jnp.int32).astype(jnp.float32)


def scale_code(bound):
    return (jnp.ceil(jnp.log2(bound) * SCALE_STEPS) + 1.0).astype(jnp.int32).astype(jnp.int16)


def scale_of(code):
    return jnp.exp2(from_code(code) * (1.0 / SCALE_STEPS))


def plan_units(n_z, tiles):
    half = tiles // 2
    plain = ((0, half, 0), (half, tiles - half, 1))
    units = []
    for step in range(n_z):
        for part, (start, count, kind) in enumerate(plain):
            units.append((step, part, start * LANES, count, kind))
    return units


def kernel(
    n_z, shard, p_dev, wedges, units,
    labels_ref, wedge_ref, x_ref, table_ref, mean_ref, total_ref,
    label_s, wedge_s, aux_own, aux_peer, x_all, table, weights, sums, inverse, tops, tallies,
    q1, r1, q2, r2, q3, r3, t3, u3,
    small_sem, load_sem, table_sem, pair_send, pair_recv, aux_send, aux_recv,
    s1, g1, s2, g2, s3, g3, ts, tg, ready,
):
    cls = lax.axis_index("cls")
    dom = lax.axis_index("dom")
    z = dom // 2
    core = lax.rem(dom, 2)
    peer = dom + 1 - 2 * core
    near = cls + 1 - 2 * lax.rem(cls, 2)
    far = cls + 2 - 4 * (cls // 2)
    both = near + 2 - 4 * (cls // 2)
    rows = 2 * p_dev
    tiles = shard // LANES
    last = n_z - 1
    offsets = sorted(range(1, n_z), key=lambda gap: -min(gap, n_z - gap)) + [0]

    def place(step):
        return lax.rem(z + offsets[step], n_z)

    small = [
        pltpu.make_async_copy(labels_ref, label_s, small_sem.at[0]),
        pltpu.make_async_copy(wedge_ref, wedge_s, small_sem.at[1]),
    ]
    for copy in small:
        copy.start()

    barrier = pltpu.get_barrier_semaphore()

    def signal(sem, who):
        pl.semaphore_signal(sem, inc=1, device_id=who, device_id_type=MESH)

    @pl.when(core == 1)
    def _():
        signal(barrier, {"dom": peer})

    loads, tables = [], []
    for step in range(n_z):
        here = place(step) * 2 + core
        span = pl.ds(pl.multiple_of(here * shard, LANES), shard)
        copy = pltpu.make_async_copy(table_ref.at[:, span], table.at[step], table_sem.at[step])
        copy.start()
        tables.append(copy)
        copies = []
        for p in range(p_dev):
            copy = pltpu.make_async_copy(
                x_ref.at[p, :, span], x_all.at[step, pl.ds(2 * p, 2)], load_sem.at[step, p]
            )
            copy.start()
            copies.append(copy)
        loads.append(copies)

    @pl.when(core == 0)
    def _():
        pl.semaphore_wait(barrier, 1)
        signal(ready, {"dom": peer})

    @pl.when(core == 1)
    def _():
        pl.semaphore_wait(ready, 1)
        signal(barrier, {"cls": near})
        signal(barrier, {"cls": far})
        for step in range(last):
            signal(barrier, {"dom": place(step) * 2 + core})

    for copy in small:
        copy.wait()
    row = lax.broadcasted_iota(jnp.int32, (rows, LANES), 0)
    lane = lax.broadcasted_iota(jnp.int32, (rows, LANES), 1)
    out_row = lax.broadcasted_iota(jnp.int32, (4 * GROUP_ROWS, LANES), 0)
    out_lane = lax.broadcasted_iota(jnp.int32, (4 * GROUP_ROWS, LANES), 1)
    wedge_of = jnp.zeros((rows, LANES), jnp.int32)
    label_of = jnp.zeros_like(out_row)
    particle = (out_lane & (rows - 1)) // 2
    for p in range(p_dev):
        wedge_of = jnp.where(row // 2 == p, wedge_s[p], wedge_of)
        label_of = jnp.where(particle == p, label_s[p], label_of)
    column = jnp.where(lane >= wedges, lane - wedges, lane)
    aux_own[0] = ((wedge_of == column) & (lane < 2 * wedges)).astype(jnp.float32)
    within = (out_row // 2) % CLASSES_PER_GROUP
    place_of = out_row // GROUP_ROWS
    for kind, order in enumerate(((cls, far, near, both), (cls, near, far, both))):
        target = jnp.zeros_like(out_row)
        for slot, group in enumerate(order):
            target = jnp.where(place_of == slot, CLASSES_PER_GROUP * group + within, target)
        aux_own[1 + kind] = (
            (target == label_of) & ((out_row & 1) == (out_lane & 1))
        ).astype(jnp.float32)

    aux_copy = pltpu.make_async_remote_copy(
        src_ref=aux_own, dst_ref=aux_peer, send_sem=aux_send, recv_sem=aux_recv,
        device_id={"dom": peer}, device_id_type=MESH,
    )
    aux_copy.start()
    pair = []
    for step in range(n_z):
        there = place(step) * 2 + (1 - core)
        span = pl.ds(pl.multiple_of(there * shard, LANES), shard)
        copies = []
        for p in range(p_dev):
            copy = pltpu.make_async_remote_copy(
                src_ref=x_ref.at[p, :, span], dst_ref=x_all.at[step, pl.ds(rows + 2 * p, 2)],
                send_sem=pair_send.at[step, p], recv_sem=pair_recv.at[step, p],
                device_id={"dom": peer}, device_id_type=MESH,
            )
            copy.start()
            copies.append(copy)
        pair.append(copies)
    aux_copy.wait()

    own_side = (out_lane & rows) == 0
    members = [
        jnp.where(own_side, aux_own[1 + kind], aux_peer[1 + kind])[:, : 4 * rows].astype(jnp.bfloat16)
        for kind in range(2)
    ]
    pick = jnp.concatenate([aux_own[0], aux_peer[0]], axis=0).astype(jnp.bfloat16)
    counts = dot(members[0][:, : 2 * rows], pick)
    pick = pick[:, : 2 * wedges]

    def send(source, target, sems, who):
        copy = pltpu.make_async_remote_copy(
            src_ref=source, dst_ref=target, send_sem=sems[0], recv_sem=sems[1],
            device_id=who, device_id_type=MESH,
        )
        copy.start()
        return copy

    def pick_weights(step):
        tables[step].wait()

        def body(span, unit):
            weights[step, :, span] = dot(pick, stack2_rows(table[step, :, span]))

        walk(0, tiles, PICK_TILES, body)

    def wire(ref, index, tally=False):
        step, part, start, count, kind = units[index]
        begin = start + part * (HEAD * LANES)
        return ref.at[step, :, pl.ds(begin, (count + 1 + tally) * LANES)]

    def head(index, extra=0):
        step, part, start, count, kind = units[index]
        return pl.ds(start + part * (HEAD * LANES) + (count + extra) * LANES, LANES)

    def shifted(span, index):
        begin = span.start + units[index][1] * (HEAD * LANES)
        return pl.ds(begin if isinstance(begin, int) else pl.multiple_of(begin, LANES), span.size)

    first, second, third, tally_copies = {}, {}, {}, []

    def compute(index):
        step, part, start, count, kind = units[index]
        if start == 0:
            for copy in loads[step] + pair[step]:
                copy.wait()
        member = members[kind]
        tops[index] = jnp.zeros((4 * GROUP_ROWS, LANES), jnp.float32)

        def body(span, unit):
            product = weights[step, :, span] * x_all[step, :, span].astype(jnp.float32)
            total = dot(member, stack2(product))
            sums[step, :, span] = total
            size = jnp.abs(total)
            pieces = [size[:, k * LANES : (k + 1) * LANES] for k in range(unit)]
            while len(pieces) > 1:
                pieces = [
                    jnp.maximum(*pieces[k : k + 2]) if k + 1 < len(pieces) else pieces[k]
                    for k in range(0, len(pieces), 2)
                ]
            tops[index] = jnp.maximum(tops[index], pieces[0])

        walk(start, count, SUM_TILES, body)
        code = scale_code(jnp.maximum(tops[index, pl.ds(PAIR_ROWS, PAIR_ROWS)], TINY))
        q1[step, :, head(index)] = code
        if index == 0:
            q1[step, :, head(index, 1)] = to_code(counts[PAIR_ROWS:])
        factor = LEVELS / scale_of(code)

        def code_body(span, unit):
            q1[step, :, shifted(span, index)] = to_code(
                sums[step, pl.ds(PAIR_ROWS, PAIR_ROWS), span] * wide(factor, unit)
            )

        walk(start, count, CODE_TILES, code_body)
        if index == 0:
            all_entered()
        partner = near if kind == 0 else far
        first[index] = send(
            wire(q1, index, index == 0), wire(r1, index, index == 0),
            (s1.at[index], g1.at[index]), {"cls": partner},
        )

    def all_entered():
        @pl.when(core == 1)
        def _():
            pl.semaphore_wait(barrier, n_z + 1)
            signal(ready, {"dom": peer})

        @pl.when(core == 0)
        def _():
            pl.semaphore_wait(ready, 1)

    def forward(index):
        step, part, start, count, kind = units[index]
        first[index].wait()
        got = scale_of(r1[step, :, head(index)])
        code = scale_code(jnp.maximum(tops[index, pl.ds(0, PAIR_ROWS)], TINY) + got)
        bound = scale_of(code)
        tops[index, pl.ds(0, PAIR_ROWS)] = bound
        q2[step, :, head(index)] = code[GROUP_ROWS:]
        if index == 0:
            tally = counts[:PAIR_ROWS] + from_code(r1[step, :, head(index, 1)])
            tallies[...] = tally
            q2[step, :, head(index, 1)] = to_code(tally)[GROUP_ROWS:]
        scale = got * (1.0 / LEVELS)
        factor = LEVELS / bound

        def body(span, unit):
            there = shifted(span, index)
            total = sums[step, pl.ds(0, PAIR_ROWS), span] + from_code(r1[step, :, there]) * wide(scale, unit)
            sums[step, pl.ds(0, PAIR_ROWS), span] = total
            q2[step, :, there] = to_code(total * wide(factor, unit))[GROUP_ROWS:]

        walk(start, count, CODE_TILES, body)
        other = far if kind == 0 else near
        second[index] = send(
            wire(q2, index, index == 0), wire(r2, index, index == 0),
            (s2.at[index], g2.at[index]), {"cls": other},
        )

    def settle(index):
        step, part, start, count, kind = units[index]
        second[index].wait()
        if index == 0:
            t3[...] = tallies[pl.ds(0, GROUP_ROWS)] + from_code(r2[step, :, head(index, 1)])
            for other in range(last):
                tally_copies.append(
                    send(t3, u3.at[other], (ts.at[other], tg.at[other]), {"dom": place(other) * 2 + core})
                )
        got = scale_of(r2[step, :, head(index)])
        scale = got * (1.0 / LEVELS)
        if step == last:

            def final_body(span, unit):
                there = shifted(span, index)
                value = sums[step, pl.ds(0, GROUP_ROWS), span] + from_code(r2[step, :, there]) * wide(scale, unit)
                mean_ref[:, span] = value * inverse[:, span]

            walk(start, count, CODE_TILES, final_body)
            return
        code = scale_code(tops[index, pl.ds(0, GROUP_ROWS)] + got)
        q3[step, :, head(index)] = code
        factor = LEVELS / scale_of(code)

        def body(span, unit):
            there = shifted(span, index)
            value = sums[step, pl.ds(0, GROUP_ROWS), span] + from_code(r2[step, :, there]) * wide(scale, unit)
            q3[step, :, there] = to_code(value * wide(factor, unit))

        walk(start, count, CODE_TILES, body)
        third[index] = send(
            wire(q3, index), wire(r3, index), (s3.at[index], g3.at[index]),
            {"dom": place(step) * 2 + core},
        )

    def gather(index):
        step, part, start, count, kind = units[index]
        mine = [k for k, unit in enumerate(units) if unit[0] < last and unit[1] == part]
        for k in mine:
            third[k].wait()
        scales = [scale_of(r3[units[k][0], :, head(k)]) * (1.0 / LEVELS) for k in mine]

        def body(span, unit):
            value = sums[step, pl.ds(0, GROUP_ROWS), span]
            for k, scale in zip(mine, scales):
                value = value + from_code(r3[units[k][0], :, shifted(span, k)]) * wide(scale, unit)
            sums[step, pl.ds(0, GROUP_ROWS), span] = value

        walk(start, count, CODE_TILES, body)

    def tally_final():
        tally = t3[...]
        for step in range(last):
            tally_copies[step].wait()
            tally = tally + u3[step]
        tally = stack2_rows(tally[:, : 2 * wedges])

        def body(span, unit):
            weight = table[last, :, span]
            total = dot(tally, stack2_rows(weight * weight))
            total = total[:GROUP_ROWS] + total[GROUP_ROWS:]
            total_ref[:, span] = total
            inverse[:, span] = 1.0 / (total + 1.0)

        walk(0, tiles, SUM_TILES, body)

    n_units = len(units)
    pick_weights(0)
    for turn in range(n_units):
        compute(turn)
        if turn + 1 < n_units and units[turn + 1][0] > units[turn][0]:
            pick_weights(units[turn + 1][0])
        if turn == 7:
            tally_final()
        if turn >= FORWARD_LAG:
            forward(turn - FORWARD_LAG)
        if turn >= SETTLE_LAG:
            settle(turn - SETTLE_LAG)
    lasts = [k for k, unit in enumerate(units) if unit[0] == last]
    pending = [k for k in range(max(0, n_units - SETTLE_LAG), n_units)]
    for k in range(max(0, n_units - FORWARD_LAG), n_units):
        forward(k)
        if pending and pending[0] not in lasts:
            settle(pending.pop(0))
    while pending and pending[0] not in lasts:
        settle(pending.pop(0))
    for k in lasts:
        gather(k)
    for k in pending:
        settle(k)


def finish(mean_ref, total_ref, avg_out, total_out):
    for index in range(avg_out.shape[0]):
        avg_out[index] = mean_ref[pl.ds(2 * index, 2)]
        total_out[pl.ds(index, 1)] = total_ref[pl.ds(2 * index, 1)]


def per_device(particles, labels, wedge_index, wedge_table):
    n_dom = lax.axis_size("dom")
    p_dev, _, voxels = particles.shape
    wedges = wedge_table.shape[0]
    shard = voxels // n_dom
    n_z = n_dom // 2
    rows = 2 * p_dev
    tiles = shard // LANES
    units = plan_units(n_z, tiles)
    count = len(units)
    any_space = pl.BlockSpec(memory_space=pl.ANY)
    vmem = pl.BlockSpec(memory_space=pltpu.VMEM)
    dma = pltpu.SemaphoreType.DMA
    f32 = jnp.float32
    scratch = [
        pltpu.SMEM((p_dev,), jnp.int32),
        pltpu.SMEM((p_dev,), jnp.int32),
        pltpu.VMEM((3, rows, LANES), f32),
        pltpu.VMEM((3, rows, LANES), f32),
        pltpu.VMEM((n_z, 2 * rows, shard), jnp.bfloat16),
        pltpu.VMEM((n_z, wedges, shard), f32),
        pltpu.VMEM((n_z, 2 * rows, shard), f32),
        pltpu.VMEM((n_z, 4 * GROUP_ROWS, shard), f32),
        pltpu.VMEM((GROUP_ROWS, shard), f32),
        pltpu.VMEM((count, 4 * GROUP_ROWS, LANES), f32),
        pltpu.VMEM((PAIR_ROWS, LANES), f32),
    ]
    long = shard + len([unit for unit in units if unit[0] == 0]) * HEAD * LANES
    for height in (PAIR_ROWS, GROUP_ROWS, GROUP_ROWS):
        scratch += [pltpu.VMEM((n_z, height, long), jnp.int16)] * 2
    scratch += [pltpu.VMEM((GROUP_ROWS, LANES), f32), pltpu.VMEM((n_z, GROUP_ROWS, LANES), f32)]
    scratch += [dma((2,)), dma((n_z, p_dev)), dma((n_z,)), dma((n_z, p_dev)), dma((n_z, p_dev)), dma, dma]
    scratch += [dma((count,))] * 6
    scratch += [dma((n_z,))] * 2 + [pltpu.SemaphoreType.REGULAR]
    mean, total = pl.pallas_call(
        functools.partial(kernel, n_z, shard, p_dev, wedges, units),
        out_shape=(
            jax.ShapeDtypeStruct((GROUP_ROWS, shard), f32),
            jax.ShapeDtypeStruct((GROUP_ROWS, shard), f32),
        ),
        in_specs=[any_space] * 4,
        out_specs=(vmem, vmem),
        scratch_shapes=scratch,
        compiler_params=pltpu.CompilerParams(
            collective_id=0, has_side_effects=True, vmem_limit_bytes=60 * 1024 * 1024
        ),
    )(labels.reshape(p_dev), wedge_index, particles, wedge_table)
    return pl.pallas_call(
        finish,
        out_shape=(
            jax.ShapeDtypeStruct((CLASSES_PER_GROUP, 2, shard), f32),
            jax.ShapeDtypeStruct((CLASSES_PER_GROUP, shard), f32),
        ),
        in_specs=[vmem, vmem],
        out_specs=(vmem, vmem),
    )(mean, total)


def solution(mesh):
    return jax.shard_map(
        per_device,
        mesh=mesh,
        in_specs=(P(("cls", "dom"), None, None), P(("cls", "dom"), None), P(("cls", "dom")), P()),
        out_specs=(P("cls", None, "dom"), P("cls", "dom")),
        check_vma=False,
    )
```

```python
import functools

import jax
import jax.numpy as jnp
from jax import lax
from jax.experimental import pallas as pl
from jax.experimental.pallas import tpu as pltpu
from jax.sharding import PartitionSpec as P

MESH = pl.DeviceIdType.MESH
LANES = 128
LEVELS = 32767.0
SCALE_STEPS = 128.0
TINY = 1e-30
HEAD = 2
CLASSES_PER_GROUP = 2
GROUP_ROWS = 2 * CLASSES_PER_GROUP
PAIR_ROWS = 2 * GROUP_ROWS
PICK_TILES = 36
SUM_TILES = 27
CODE_TILES = 27
FORWARD_LAG = 2
SETTLE_LAG = 4


def divisor(number, cap):
    return max(size for size in range(1, cap + 1) if number % size == 0)


def dot(left, right):
    return jnp.dot(left, right, preferred_element_type=jnp.float32)


def stack2(value):
    high = value.astype(jnp.bfloat16)
    low = (value - high.astype(jnp.float32)).astype(jnp.bfloat16)
    return jnp.concatenate([high, low], axis=0)


def stack2_rows(value):
    high = value.astype(jnp.bfloat16).astype(jnp.float32)
    return jnp.concatenate([high, value - high], axis=0).astype(jnp.bfloat16)


def walk(start, tiles, cap, body):
    unit = divisor(tiles, cap)
    turns = tiles // unit
    if turns == 1:
        body(pl.ds(start, unit * LANES), unit)
        return

    @pl.loop(0, turns)
    def _(index):
        body(pl.ds(pl.multiple_of(start + index * (unit * LANES), LANES), unit * LANES), unit)


def wide(value, unit):
    return jnp.concatenate([value] * unit, axis=1) if unit > 1 else value


def to_code(value):
    return jnp.round(value).astype(jnp.int32).astype(jnp.int16)


def from_code(code):
    return code.astype(jnp.int32).astype(jnp.float32)


def scale_code(bound):
    return (jnp.ceil(jnp.log2(bound) * SCALE_STEPS) + 1.0).astype(jnp.int32).astype(jnp.int16)


def scale_of(code):
    return jnp.exp2(from_code(code) * (1.0 / SCALE_STEPS))


def plan_units(n_z, tiles):
    half = tiles // 2
    plain = ((0, half, 0), (half, tiles - half, 1))
    units = []
    for step in range(n_z):
        for part, (start, count, kind) in enumerate(plain):
            units.append((step, part, start * LANES, count, kind))
    return units


def kernel(
    n_z, shard, p_dev, wedges, units,
    labels_ref, wedge_ref, x_ref, table_ref, mean_ref, total_ref,
    label_s, wedge_s, aux_own, aux_peer, x_all, table, weights, sums, inverse, tops, tallies,
    q1, r1, q2, r2, q3, r3, t3, u3,
    small_sem, load_sem, table_sem, pair_send, pair_recv, aux_send, aux_recv,
    s1, g1, s2, g2, s3, g3, ts, tg, ready, up, down,
):
    cls = lax.axis_index("cls")
    dom = lax.axis_index("dom")
    z = dom // 2
    core = lax.rem(dom, 2)
    peer = dom + 1 - 2 * core
    near = cls + 1 - 2 * lax.rem(cls, 2)
    far = cls + 2 - 4 * (cls // 2)
    both = near + 2 - 4 * (cls // 2)
    rows = 2 * p_dev
    tiles = shard // LANES
    last = n_z - 1
    offsets = sorted(range(1, n_z), key=lambda gap: -min(gap, n_z - gap)) + [0]

    def place(step):
        return lax.rem(z + offsets[step], n_z)

    small = [
        pltpu.make_async_copy(labels_ref, label_s, small_sem.at[0]),
        pltpu.make_async_copy(wedge_ref, wedge_s, small_sem.at[1]),
    ]
    for copy in small:
        copy.start()

    barrier = pltpu.get_barrier_semaphore()

    def signal(sem, who):
        pl.semaphore_signal(sem, inc=1, device_id=who, device_id_type=MESH)

    @pl.when(core == 1)
    def _():
        signal(barrier, {"dom": peer})

    loads, tables = [], []
    for step in range(n_z):
        here = place(step) * 2 + core
        span = pl.ds(pl.multiple_of(here * shard, LANES), shard)
        copy = pltpu.make_async_copy(table_ref.at[:, span], table.at[step], table_sem.at[step])
        copy.start()
        tables.append(copy)
        copies = []
        for p in range(p_dev):
            copy = pltpu.make_async_copy(
                x_ref.at[p, :, span], x_all.at[step, pl.ds(2 * p, 2)], load_sem.at[step, p]
            )
            copy.start()
            copies.append(copy)
        loads.append(copies)

    @pl.when(core == 0)
    def _():
        pl.semaphore_wait(barrier, 1)
        signal(ready, {"dom": peer})

    @pl.when(core == 1)
    def _():
        pl.semaphore_wait(ready, 1)
        signal(barrier, {"cls": near})
        signal(barrier, {"cls": far})

        @pl.when(z > 0)
        def _():
            signal(barrier, {"dom": dom - 2})

        @pl.when(z < last)
        def _():
            signal(barrier, {"dom": dom + 2})


    for copy in small:
        copy.wait()
    row = lax.broadcasted_iota(jnp.int32, (rows, LANES), 0)
    lane = lax.broadcasted_iota(jnp.int32, (rows, LANES), 1)
    out_row = lax.broadcasted_iota(jnp.int32, (4 * GROUP_ROWS, LANES), 0)
    out_lane = lax.broadcasted_iota(jnp.int32, (4 * GROUP_ROWS, LANES), 1)
    wedge_of = jnp.zeros((rows, LANES), jnp.int32)
    label_of = jnp.zeros_like(out_row)
    particle = (out_lane & (rows - 1)) // 2
    for p in range(p_dev):
        wedge_of = jnp.where(row // 2 == p, wedge_s[p], wedge_of)
        label_of = jnp.where(particle == p, label_s[p], label_of)
    column = jnp.where(lane >= wedges, lane - wedges, lane)
    aux_own[0] = ((wedge_of == column) & (lane < 2 * wedges)).astype(jnp.float32)
    within = (out_row // 2) % CLASSES_PER_GROUP
    place_of = out_row // GROUP_ROWS
    for kind, order in enumerate(((cls, far, near, both), (cls, near, far, both))):
        target = jnp.zeros_like(out_row)
        for slot, group in enumerate(order):
            target = jnp.where(place_of == slot, CLASSES_PER_GROUP * group + within, target)
        aux_own[1 + kind] = (
            (target == label_of) & ((out_row & 1) == (out_lane & 1))
        ).astype(jnp.float32)

    aux_copy = pltpu.make_async_remote_copy(
        src_ref=aux_own, dst_ref=aux_peer, send_sem=aux_send, recv_sem=aux_recv,
        device_id={"dom": peer}, device_id_type=MESH,
    )
    aux_copy.start()
    pair = []
    for step in range(n_z):
        there = place(step) * 2 + (1 - core)
        span = pl.ds(pl.multiple_of(there * shard, LANES), shard)
        copies = []
        for p in range(p_dev):
            copy = pltpu.make_async_remote_copy(
                src_ref=x_ref.at[p, :, span], dst_ref=x_all.at[step, pl.ds(rows + 2 * p, 2)],
                send_sem=pair_send.at[step, p], recv_sem=pair_recv.at[step, p],
                device_id={"dom": peer}, device_id_type=MESH,
            )
            copy.start()
            copies.append(copy)
        pair.append(copies)
    aux_copy.wait()

    own_side = (out_lane & rows) == 0
    members = [
        jnp.where(own_side, aux_own[1 + kind], aux_peer[1 + kind])[:, : 4 * rows].astype(jnp.bfloat16)
        for kind in range(2)
    ]
    pick = jnp.concatenate([aux_own[0], aux_peer[0]], axis=0).astype(jnp.bfloat16)
    counts = dot(members[0][:, : 2 * rows], pick)
    pick = pick[:, : 2 * wedges]

    def send(source, target, sems, who):
        copy = pltpu.make_async_remote_copy(
            src_ref=source, dst_ref=target, send_sem=sems[0], recv_sem=sems[1],
            device_id=who, device_id_type=MESH,
        )
        copy.start()
        return copy

    def pick_weights(step):
        tables[step].wait()

        def body(span, unit):
            weights[step, :, span] = dot(pick, stack2_rows(table[step, :, span]))

        walk(0, tiles, PICK_TILES, body)

    def wire(ref, index, tally=False):
        step, part, start, count, kind = units[index]
        begin = start + part * (HEAD * LANES)
        return ref.at[step, :, pl.ds(begin, (count + 1 + tally) * LANES)]

    def head(index, extra=0):
        step, part, start, count, kind = units[index]
        return pl.ds(start + part * (HEAD * LANES) + (count + extra) * LANES, LANES)

    def shifted(span, index):
        begin = span.start + units[index][1] * (HEAD * LANES)
        return pl.ds(begin if isinstance(begin, int) else pl.multiple_of(begin, LANES), span.size)

    first, second, third, tally_copies = {}, {}, {}, []

    def compute(index):
        step, part, start, count, kind = units[index]
        if start == 0:
            for copy in loads[step] + pair[step]:
                copy.wait()
        member = members[kind]
        tops[index] = jnp.zeros((4 * GROUP_ROWS, LANES), jnp.float32)

        def body(span, unit):
            product = weights[step, :, span] * x_all[step, :, span].astype(jnp.float32)
            total = dot(member, stack2(product))
            sums[step, :, span] = total
            size = jnp.abs(total)
            pieces = [size[:, k * LANES : (k + 1) * LANES] for k in range(unit)]
            while len(pieces) > 1:
                pieces = [
                    jnp.maximum(*pieces[k : k + 2]) if k + 1 < len(pieces) else pieces[k]
                    for k in range(0, len(pieces), 2)
                ]
            tops[index] = jnp.maximum(tops[index], pieces[0])

        walk(start, count, SUM_TILES, body)
        code = scale_code(jnp.maximum(tops[index, pl.ds(PAIR_ROWS, PAIR_ROWS)], TINY))
        q1[step, :, head(index)] = code
        if index == 0:
            q1[step, :, head(index, 1)] = to_code(counts[PAIR_ROWS:])
        factor = LEVELS / scale_of(code)

        def code_body(span, unit):
            q1[step, :, shifted(span, index)] = to_code(
                sums[step, pl.ds(PAIR_ROWS, PAIR_ROWS), span] * wide(factor, unit)
            )

        walk(start, count, CODE_TILES, code_body)
        if index == 0:
            all_entered()
        partner = near if kind == 0 else far
        first[index] = send(
            wire(q1, index, index == 0), wire(r1, index, index == 0),
            (s1.at[index], g1.at[index]), {"cls": partner},
        )

    def all_entered():
        @pl.when(core == 1)
        def _():
            pl.semaphore_wait(barrier, 2 + jnp.minimum(z, 1) + jnp.minimum(last - z, 1))
            signal(ready, {"dom": peer})

        @pl.when(core == 0)
        def _():
            pl.semaphore_wait(ready, 1)

    def tell(gap):
        @pl.when((core == 1) & (z > 0) & (z + gap - 1 <= last))
        def _():
            signal(up.at[gap], {"dom": dom - 2})

        @pl.when((core == 1) & (z < last) & (z - gap + 1 >= 0))
        def _():
            signal(down.at[gap], {"dom": dom + 2})

    def hear(gap):
        @pl.when((core == 1) & (z + gap <= last))
        def _():
            pl.semaphore_wait(up.at[gap], 1)

        @pl.when((core == 1) & (z - gap >= 0))
        def _():
            pl.semaphore_wait(down.at[gap], 1)

    rounds = [functools.partial(tell, 2)] if last >= 2 else []
    for gap in range(2, last + 1):
        rounds.append(functools.partial(hear, gap))
        if gap < last:
            rounds.append(functools.partial(tell, gap + 1))

    def column_entered():
        while rounds:
            rounds.pop(0)()

        @pl.when(core == 1)
        def _():
            signal(ready, {"dom": peer})

        @pl.when(core == 0)
        def _():
            pl.semaphore_wait(ready, 1)

    def forward(index):
        step, part, start, count, kind = units[index]
        first[index].wait()
        got = scale_of(r1[step, :, head(index)])
        code = scale_code(jnp.maximum(tops[index, pl.ds(0, PAIR_ROWS)], TINY) + got)
        bound = scale_of(code)
        tops[index, pl.ds(0, PAIR_ROWS)] = bound
        q2[step, :, head(index)] = code[GROUP_ROWS:]
        if index == 0:
            tally = counts[:PAIR_ROWS] + from_code(r1[step, :, head(index, 1)])
            tallies[...] = tally
            q2[step, :, head(index, 1)] = to_code(tally)[GROUP_ROWS:]
        scale = got * (1.0 / LEVELS)
        factor = LEVELS / bound

        def body(span, unit):
            there = shifted(span, index)
            total = sums[step, pl.ds(0, PAIR_ROWS), span] + from_code(r1[step, :, there]) * wide(scale, unit)
            sums[step, pl.ds(0, PAIR_ROWS), span] = total
            q2[step, :, there] = to_code(total * wide(factor, unit))[GROUP_ROWS:]

        walk(start, count, CODE_TILES, body)
        other = far if kind == 0 else near
        second[index] = send(
            wire(q2, index, index == 0), wire(r2, index, index == 0),
            (s2.at[index], g2.at[index]), {"cls": other},
        )

    def settle(index):
        step, part, start, count, kind = units[index]
        second[index].wait()
        if index == 0:
            column_entered()
            t3[...] = tallies[pl.ds(0, GROUP_ROWS)] + from_code(r2[step, :, head(index, 1)])
            for other in range(last):
                tally_copies.append(
                    send(t3, u3.at[other], (ts.at[other], tg.at[other]), {"dom": place(other) * 2 + core})
                )
        got = scale_of(r2[step, :, head(index)])
        scale = got * (1.0 / LEVELS)
        if step == last:

            def final_body(span, unit):
                there = shifted(span, index)
                value = sums[step, pl.ds(0, GROUP_ROWS), span] + from_code(r2[step, :, there]) * wide(scale, unit)
                mean_ref[:, span] = value * inverse[:, span]

            walk(start, count, CODE_TILES, final_body)
            return
        code = scale_code(tops[index, pl.ds(0, GROUP_ROWS)] + got)
        q3[step, :, head(index)] = code
        factor = LEVELS / scale_of(code)

        def body(span, unit):
            there = shifted(span, index)
            value = sums[step, pl.ds(0, GROUP_ROWS), span] + from_code(r2[step, :, there]) * wide(scale, unit)
            q3[step, :, there] = to_code(value * wide(factor, unit))

        walk(start, count, CODE_TILES, body)
        third[index] = send(
            wire(q3, index), wire(r3, index), (s3.at[index], g3.at[index]),
            {"dom": place(step) * 2 + core},
        )

    def gather(index):
        step, part, start, count, kind = units[index]
        mine = [k for k, unit in enumerate(units) if unit[0] < last and unit[1] == part]
        for k in mine:
            third[k].wait()
        scales = [scale_of(r3[units[k][0], :, head(k)]) * (1.0 / LEVELS) for k in mine]

        def body(span, unit):
            value = sums[step, pl.ds(0, GROUP_ROWS), span]
            for k, scale in zip(mine, scales):
                value = value + from_code(r3[units[k][0], :, shifted(span, k)]) * wide(scale, unit)
            sums[step, pl.ds(0, GROUP_ROWS), span] = value

        walk(start, count, CODE_TILES, body)

    def tally_final():
        tally = t3[...]
        for step in range(last):
            tally_copies[step].wait()
            tally = tally + u3[step]
        tally = stack2_rows(tally[:, : 2 * wedges])

        def body(span, unit):
            weight = table[last, :, span]
            total = dot(tally, stack2_rows(weight * weight))
            total = total[:GROUP_ROWS] + total[GROUP_ROWS:]
            total_ref[:, span] = total
            inverse[:, span] = 1.0 / (total + 1.0)

        walk(0, tiles, SUM_TILES, body)

    n_units = len(units)
    pick_weights(0)
    for turn in range(n_units):
        compute(turn)
        for _ in range(min(len(rounds), 2 if turn else 1)):
            rounds.pop(0)()
        if turn + 1 < n_units and units[turn + 1][0] > units[turn][0]:
            pick_weights(units[turn + 1][0])
        if turn == 7:
            tally_final()
        if turn >= FORWARD_LAG:
            forward(turn - FORWARD_LAG)
        if turn >= SETTLE_LAG:
            settle(turn - SETTLE_LAG)
    lasts = [k for k, unit in enumerate(units) if unit[0] == last]
    pending = [k for k in range(max(0, n_units - SETTLE_LAG), n_units)]
    for k in range(max(0, n_units - FORWARD_LAG), n_units):
        forward(k)
        if pending and pending[0] not in lasts:
            settle(pending.pop(0))
    while pending and pending[0] not in lasts:
        settle(pending.pop(0))
    for k in lasts:
        gather(k)
    for k in pending:
        settle(k)


def finish(mean_ref, total_ref, avg_out, total_out, sem):
    copies = []
    for index in range(avg_out.shape[0]):
        copies.append(
            pltpu.make_async_copy(mean_ref.at[pl.ds(2 * index, 2)], avg_out.at[index], sem.at[2 * index])
        )
        copies.append(
            pltpu.make_async_copy(
                total_ref.at[pl.ds(2 * index, 1)], total_out.at[pl.ds(index, 1)], sem.at[2 * index + 1]
            )
        )
    for copy in copies:
        copy.start()
    for copy in copies:
        copy.wait()


def per_device(particles, labels, wedge_index, wedge_table):
    n_dom = lax.axis_size("dom")
    p_dev, _, voxels = particles.shape
    wedges = wedge_table.shape[0]
    shard = voxels // n_dom
    n_z = n_dom // 2
    rows = 2 * p_dev
    tiles = shard // LANES
    units = plan_units(n_z, tiles)
    count = len(units)
    any_space = pl.BlockSpec(memory_space=pl.ANY)
    vmem = pl.BlockSpec(memory_space=pltpu.VMEM)
    dma = pltpu.SemaphoreType.DMA
    f32 = jnp.float32
    scratch = [
        pltpu.SMEM((p_dev,), jnp.int32),
        pltpu.SMEM((p_dev,), jnp.int32),
        pltpu.VMEM((3, rows, LANES), f32),
        pltpu.VMEM((3, rows, LANES), f32),
        pltpu.VMEM((n_z, 2 * rows, shard), jnp.bfloat16),
        pltpu.VMEM((n_z, wedges, shard), f32),
        pltpu.VMEM((n_z, 2 * rows, shard), f32),
        pltpu.VMEM((n_z, 4 * GROUP_ROWS, shard), f32),
        pltpu.VMEM((GROUP_ROWS, shard), f32),
        pltpu.VMEM((count, 4 * GROUP_ROWS, LANES), f32),
        pltpu.VMEM((PAIR_ROWS, LANES), f32),
    ]
    long = shard + len([unit for unit in units if unit[0] == 0]) * HEAD * LANES
    for height in (PAIR_ROWS, GROUP_ROWS, GROUP_ROWS):
        scratch += [pltpu.VMEM((n_z, height, long), jnp.int16)] * 2
    scratch += [pltpu.VMEM((GROUP_ROWS, LANES), f32), pltpu.VMEM((n_z, GROUP_ROWS, LANES), f32)]
    scratch += [dma((2,)), dma((n_z, p_dev)), dma((n_z,)), dma((n_z, p_dev)), dma((n_z, p_dev)), dma, dma]
    scratch += [dma((count,))] * 6
    scratch += [dma((n_z,))] * 2 + [pltpu.SemaphoreType.REGULAR]
    scratch += [pltpu.SemaphoreType.REGULAR((n_z,))] * 2
    mean, total = pl.pallas_call(
        functools.partial(kernel, n_z, shard, p_dev, wedges, units),
        out_shape=(
            pltpu.VMEM((GROUP_ROWS, shard), f32),
            pltpu.VMEM((GROUP_ROWS, shard), f32),
        ),
        in_specs=[any_space] * 4,
        out_specs=(vmem, vmem),
        scratch_shapes=scratch,
        compiler_params=pltpu.CompilerParams(
            collective_id=0, has_side_effects=True, vmem_limit_bytes=60 * 1024 * 1024
        ),
    )(labels.reshape(p_dev), wedge_index, particles, wedge_table)
    return pl.pallas_call(
        finish,
        out_shape=(
            jax.ShapeDtypeStruct((CLASSES_PER_GROUP, 2, shard), f32),
            jax.ShapeDtypeStruct((CLASSES_PER_GROUP, shard), f32),
        ),
        in_specs=[any_space, any_space],
        out_specs=(any_space, any_space),
        compiler_params=pltpu.CompilerParams(vmem_limit_bytes=4 * 1024 * 1024),
        scratch_shapes=[dma((2 * CLASSES_PER_GROUP,))],
    )(mean, total)


def solution(mesh):
    return jax.shard_map(
        per_device,
        mesh=mesh,
        in_specs=(P(("cls", "dom"), None, None), P(("cls", "dom"), None), P(("cls", "dom")), P()),
        out_specs=(P("cls", None, "dom"), P("cls", "dom")),
        check_vma=False,
    )
```

```python
import functools

import jax
import jax.numpy as jnp
from jax import lax
from jax.experimental import pallas as pl
from jax.experimental.pallas import tpu as pltpu
from jax.sharding import PartitionSpec as P

MESH = pl.DeviceIdType.MESH
LANES = 128
LEVELS = 32767.0
SCALE_STEPS = 128.0
TINY = 1e-30
HEAD = 2
CLASSES_PER_GROUP = 2
GROUP_ROWS = 2 * CLASSES_PER_GROUP
PAIR_ROWS = 2 * GROUP_ROWS
PICK_TILES = 108
SUM_TILES = 54
CODE_TILES = 27
AHEAD = 2
SETTLE_AFTER = 1
OWN_PAIRS = 2
EARLY_SHARE = 0.45


def divisor(number, cap):
    return max(size for size in range(1, cap + 1) if number % size == 0)


def padded(count):
    return -(-count // 16) * 16


def filled(value):
    extra = padded(value.shape[0]) - value.shape[0]
    if extra == 0:
        return value
    return jnp.concatenate([value, jnp.zeros((extra, value.shape[1]), value.dtype)], axis=0)


def dot(left, right):
    return jnp.dot(left, right, preferred_element_type=jnp.float32)


def stack2(value):
    high = value.astype(jnp.bfloat16)
    low = (value - high.astype(jnp.float32)).astype(jnp.bfloat16)
    return jnp.concatenate([high, low], axis=0)


def walk(start, tiles, cap, body):
    unit = divisor(tiles, cap)
    turns = tiles // unit
    if turns == 1:
        body(pl.ds(start, unit * LANES), unit)
        return

    @pl.loop(0, turns)
    def _(index):
        body(pl.ds(pl.multiple_of(start + index * (unit * LANES), LANES), unit * LANES), unit)


def wide(value, unit):
    return jnp.concatenate([value] * unit, axis=1) if unit > 1 else value


def to_code(value):
    return jnp.round(value).astype(jnp.int32).astype(jnp.int16)


def from_code(code):
    return code.astype(jnp.int32).astype(jnp.float32)


def scale_code(bound):
    return (jnp.ceil(jnp.log2(bound) * SCALE_STEPS) + 1.0).astype(jnp.int32).astype(jnp.int16)


def scale_of(code):
    return jnp.exp2(from_code(code) * (1.0 / SCALE_STEPS))


def plan_units(n_z, tiles):
    half = tiles // 2
    early = int(tiles * EARLY_SHARE / 2)
    units, pairs, firsts = [], [], []

    def add(step, pieces, early=False):
        base = sum(1 for unit in units if unit[0] == step)
        names = []
        for part, (start, count, kind) in enumerate(pieces):
            names.append(len(units))
            units.append((step, base + part, start * LANES, count, kind, early))
        return names

    for step in range(n_z):
        if step == n_z - 2 and early:
            firsts = add(step, ((0, early, 0), (half, early, 1)), True)
            pairs.append(add(step, ((early, half - early, 0), (half + early, tiles - half - early, 1))))
        elif step == n_z - 1 and OWN_PAIRS == 2 and half >= 2:
            cut = half // 2
            pairs.append(add(step, ((0, cut, 0), (half, cut, 1))))
            pairs.append(add(step, ((cut, half - cut, 0), (half + cut, tiles - half - cut, 1))))
        else:
            pairs.append(add(step, ((0, half, 0), (half, tiles - half, 1))))
    starts = [sorted(unit[2] for unit in units if unit[0] == step) for step in range(n_z)]
    units = [(unit[0], starts[unit[0]].index(unit[2]), *unit[2:]) for unit in units]
    return units, pairs, firsts


def plan_order(n_z, units, pairs, firsts):
    order, count = [], len(pairs)
    own = [k for k, unit in enumerate(units) if unit[0] == n_z - 1]
    ready = set()

    def weights(step):
        if step not in ready:
            ready.add(step)
            order.append(("P", step))

    def compute(j):
        if j < count:
            weights(units[pairs[j][0]][0])
            order.extend(("C", k) for k in pairs[j])

    compute(0)
    if firsts:
        weights(n_z - 2)
        order.extend(("Z", k) for k in firsts)
    for j in range(1, AHEAD):
        compute(j)
    for j in range(count):
        order.extend(("F", k) for k in pairs[j])
        compute(j + AHEAD)
        if j >= SETTLE_AFTER:
            order.extend(("S", k) for k in pairs[j - SETTLE_AFTER] if k not in own)
    late = [k for pair in pairs[count - SETTLE_AFTER :] for k in pair]
    remote = [k for k, unit in enumerate(units) if unit[0] < n_z - 1 and not unit[5]]
    order.extend(("S", k) for k in late if k not in own)
    order.append(("T", 0))
    order.extend(("G", k) for k in remote)
    order.extend(("S", k) for k in own)
    return order


def kernel(
    n_z, shard, p_dev, wedges, units, script,
    labels_ref, wedge_ref, x_ref, table_ref, mean_ref, total_ref,
    label_s, wedge_s, aux_own, aux_peer, x_all, table, weights, sums, inverse, tops, tallies,
    q0, r0, q1, r1, q2, r2, q3, r3, t3, u3,
    small_sem, load_sem, table_sem, pair_send, pair_recv, aux_send, aux_recv,
    s0, g0, s1, g1, g2, g3, ts, tg, ready, up, down,
):
    cls = lax.axis_index("cls")
    dom = lax.axis_index("dom")
    z = dom // 2
    core = lax.rem(dom, 2)
    peer = dom + 1 - 2 * core
    near = cls + 1 - 2 * lax.rem(cls, 2)
    far = cls + 2 - 4 * (cls // 2)
    both = near + 2 - 4 * (cls // 2)
    rows = 2 * p_dev
    tiles = shard // LANES
    last = n_z - 1
    slots = padded(wedges)
    offsets = sorted(range(1, n_z), key=lambda gap: -min(gap, n_z - gap)) + [0]

    def place(step):
        return lax.rem(z + offsets[step], n_z)

    small = [
        pltpu.make_async_copy(labels_ref, label_s, small_sem.at[0]),
        pltpu.make_async_copy(wedge_ref, wedge_s, small_sem.at[1]),
    ]
    for copy in small:
        copy.start()

    barrier = pltpu.get_barrier_semaphore()

    def signal(sem, who):
        pl.semaphore_signal(sem, inc=1, device_id=who, device_id_type=MESH)

    @pl.when(core == 1)
    def _():
        signal(barrier, {"dom": peer})

    loads, tables, pair = [], [], []

    def chunks(step, where):
        base = (place(step) * 2 + where) * shard
        cut = tiles // 2 * LANES if step == 0 else 0
        spans = [(0, cut), (cut, shard - cut)] if cut else [(0, shard)]
        return [
            (pl.ds(pl.multiple_of(base + begin, LANES), size), pl.ds(begin, size))
            for begin, size in spans
        ]

    def load_step(step):
        here = place(step) * 2 + core
        span = pl.ds(pl.multiple_of(here * shard, LANES), shard)
        copy = pltpu.make_async_copy(
            table_ref.at[:, span], table.at[step], table_sem.at[step]
        )
        copy.start()
        tables.append(copy)
        waits = []
        for part, (source, target) in enumerate(chunks(step, core)):
            for p in range(p_dev):
                pltpu.make_async_copy(
                    x_ref.at[p, :, source], x_all.at[step, pl.ds(2 * p, 2), target],
                    load_sem.at[step, part],
                ).start()
            block = x_all.at[step, pl.ds(0, rows), target]
            waits.append(pltpu.make_async_copy(block, block, load_sem.at[step, part]))
        loads.append(waits)

    def pair_step(step):
        waits = []
        for part, (source, target) in enumerate(chunks(step, 1 - core)):
            def pair_copy(source, target):
                return pltpu.make_async_remote_copy(
                    src_ref=source, dst_ref=target,
                    send_sem=pair_send, recv_sem=pair_recv.at[step, part],
                    device_id={"dom": peer}, device_id_type=MESH,
                )

            for p in range(p_dev):
                pair_copy(
                    x_ref.at[p, :, source], x_all.at[step, pl.ds(rows + 2 * p, 2), target]
                ).start()
            block = x_all.at[step, pl.ds(rows, rows), target]
            waits.append(pair_copy(block, block))
        pair.append(waits)

    for step in range(n_z):
        load_step(step)

    @pl.when(core == 0)
    def _():
        pl.semaphore_wait(barrier, 1)
        signal(ready, {"dom": peer})

    @pl.when(core == 1)
    def _():
        pl.semaphore_wait(ready, 1)
        signal(barrier, {"cls": near})
        signal(barrier, {"cls": far})

        @pl.when(z > 0)
        def _():
            signal(barrier, {"dom": dom - 2})

        @pl.when(z < last)
        def _():
            signal(barrier, {"dom": dom + 2})


    for copy in small:
        copy.wait()
    row = lax.broadcasted_iota(jnp.int32, (rows, LANES), 0)
    lane = lax.broadcasted_iota(jnp.int32, (rows, LANES), 1)
    out_row = lax.broadcasted_iota(jnp.int32, (4 * GROUP_ROWS, LANES), 0)
    out_lane = lax.broadcasted_iota(jnp.int32, (4 * GROUP_ROWS, LANES), 1)
    wedge_of = jnp.zeros((rows, LANES), jnp.int32)
    label_of = jnp.zeros_like(out_row)
    particle = (out_lane & (rows - 1)) // 2
    for p in range(p_dev):
        wedge_of = jnp.where(row // 2 == p, wedge_s[p], wedge_of)
        label_of = jnp.where(particle == p, label_s[p], label_of)
    column = jnp.where(lane >= slots, lane - slots, lane)
    aux_own[0] = ((wedge_of == column) & (lane < 2 * slots)).astype(jnp.float32)
    within = (out_row // 2) % CLASSES_PER_GROUP
    place_of = out_row // GROUP_ROWS
    for kind, order in enumerate(((cls, far, near, both), (cls, near, far, both))):
        target = jnp.zeros_like(out_row)
        for slot, group in enumerate(order):
            target = jnp.where(place_of == slot, CLASSES_PER_GROUP * group + within, target)
        aux_own[1 + kind] = (
            (target == label_of) & ((out_row & 1) == (out_lane & 1))
        ).astype(jnp.float32)

    aux_copy = pltpu.make_async_remote_copy(
        src_ref=aux_own, dst_ref=aux_peer, send_sem=aux_send, recv_sem=aux_recv,
        device_id={"dom": peer}, device_id_type=MESH,
    )
    aux_copy.start()
    for step in range(n_z):
        pair_step(step)
    aux_copy.wait()

    own_side = (out_lane & rows) == 0
    members = [
        jnp.where(own_side, aux_own[1 + kind], aux_peer[1 + kind])[:, : 4 * rows].astype(jnp.bfloat16)
        for kind in range(2)
    ]
    pick = jnp.concatenate([aux_own[0], aux_peer[0]], axis=0).astype(jnp.bfloat16)
    counts = dot(members[0][:, : 2 * rows], pick)
    pick = pick[:, : 2 * slots]

    def send(source, target, sems, who):
        copy = pltpu.make_async_remote_copy(
            src_ref=source, dst_ref=target, send_sem=sems[0], recv_sem=sems[1],
            device_id=who, device_id_type=MESH,
        )
        copy.start()
        return copy

    def pick_weights(step):
        tables[step].wait()

        def body(span, unit):
            weights[step, :, span] = dot(pick, stack2(filled(table[step, :, span])))

        walk(0, tiles, PICK_TILES, body)

    def wire(ref, index, tally=False):
        step, part, start, count, kind, _ = units[index]
        begin = start + part * (HEAD * LANES)
        return ref.at[step, :, pl.ds(begin, (count + 1 + tally) * LANES)]

    def head(index, extra=0):
        step, part, start, count, kind, _ = units[index]
        return pl.ds(start + part * (HEAD * LANES) + (count + extra) * LANES, LANES)

    def shifted(span, index):
        begin = span.start + units[index][1] * (HEAD * LANES)
        return pl.ds(begin if isinstance(begin, int) else pl.multiple_of(begin, LANES), span.size)

    zeroth, first, second, third, tally_copies = {}, {}, {}, {}, []
    column_known = []

    def pieces_of(index):
        step, part, start, count, kind, _ = units[index]
        if step != last:
            return [(start, count, None)]
        pieces, at, end = [], start, start + count * LANES
        for k, unit in enumerate(units):
            low, high = max(at, unit[2]), min(end, unit[2] + unit[3] * LANES)
            if unit[5] and low < high:
                if low > at:
                    pieces.append((at, (low - at) // LANES, None))
                pieces.append((low, (high - low) // LANES, k))
                at = high
        if at < end:
            pieces.append((at, (end - at) // LANES, None))
        return pieces

    def number(index):
        return index - len([k for k in range(index) if units[k][5]])

    def early_slot(index):
        slot = [k for k, unit in enumerate(units) if unit[5]].index(index)
        return slot, (units[index][3] + 1) * LANES

    def early_wire(ref, index):
        slot, size = early_slot(index)
        return ref.at[slot, :, pl.ds(0, size)]

    loaded, landed = set(), set()

    def compute(index):
        step, part, start, count, kind, early = units[index]
        groups = len(loads[step])
        for group in range(1 if groups > 1 and start + count * LANES <= tiles // 2 * LANES else groups):
            if (step, group) not in loaded:
                loaded.add((step, group))
                loads[step][group].wait()
                pair[step][group].wait_recv()
        member = members[kind]
        tops[index] = jnp.zeros((4 * GROUP_ROWS, LANES), jnp.float32)
        for begin, length, source in pieces_of(index):
            scale = None
            if source is not None:
                slot = early_slot(source)[0]
                if source not in landed:
                    landed.add(source)
                    zeroth[source].wait()
                origin = units[source][2]
                scale = scale_of(r0[slot, :, pl.ds(units[source][3] * LANES, LANES)]) * (1.0 / LEVELS)

            def body(span, unit):
                product = weights[step, :, span] * x_all[step, :, span].astype(jnp.float32)
                total = dot(member, stack2(product))
                if scale is not None:
                    at = span.start - origin
                    there = pl.ds(at if isinstance(at, int) else pl.multiple_of(at, LANES), span.size)
                    total = total + from_code(r0[slot, :, there]) * wide(scale, unit)
                sums[step, :, span] = total
                size = jnp.abs(total)
                parts = [size[:, k * LANES : (k + 1) * LANES] for k in range(unit)]
                while len(parts) > 1:
                    parts = [
                        jnp.maximum(*parts[k : k + 2]) if k + 1 < len(parts) else parts[k]
                        for k in range(0, len(parts), 2)
                    ]
                tops[index] = jnp.maximum(tops[index], parts[0])

            walk(begin, length, SUM_TILES, body)
        span = pl.ds(start, count * LANES)
        if early:
            slot, size = early_slot(index)
            code = scale_code(jnp.maximum(tops[index], TINY))
            q0[slot, :, pl.ds(count * LANES, LANES)] = code
            factor = LEVELS / scale_of(code)

            def early_body(span, unit):
                at = span.start - start
                there = pl.ds(at if isinstance(at, int) else pl.multiple_of(at, LANES), span.size)
                q0[slot, :, there] = to_code(sums[step, :, span] * wide(factor, unit))

            walk(start, count, CODE_TILES, early_body)
            column_entered()
            zeroth[index] = send(
                early_wire(q0, index), early_wire(r0, index), (s0.at[slot], g0.at[slot]),
                {"dom": place(step) * 2 + core},
            )
            return
        code = scale_code(jnp.maximum(tops[index, pl.ds(PAIR_ROWS, PAIR_ROWS)], TINY))
        q1[step, :, head(index)] = code
        if index == 0:
            q1[step, :, head(index, 1)] = to_code(counts[PAIR_ROWS:])
        factor = LEVELS / scale_of(code)

        def code_body(span, unit):
            q1[step, :, shifted(span, index)] = to_code(
                sums[step, pl.ds(PAIR_ROWS, PAIR_ROWS), span] * wide(factor, unit)
            )

        walk(start, count, CODE_TILES, code_body)
        if index == 0:
            all_entered()
        partner = near if kind == 0 else far
        first[index] = send(
            wire(q1, index, index == 0), wire(r1, index, index == 0),
            (s1.at[number(index)], g1.at[number(index)]), {"cls": partner},
        )

    def all_entered():
        @pl.when(core == 1)
        def _():
            pl.semaphore_wait(barrier, 2 + jnp.minimum(z, 1) + jnp.minimum(last - z, 1))
            signal(ready, {"dom": peer})

        @pl.when(core == 0)
        def _():
            pl.semaphore_wait(ready, 1)

    def tell(gap):
        @pl.when((core == 1) & (z > 0) & (z + gap - 1 <= last))
        def _():
            signal(up.at[gap - 2], {"dom": dom - 2})

        @pl.when((core == 1) & (z < last) & (z - gap + 1 >= 0))
        def _():
            signal(down.at[gap - 2], {"dom": dom + 2})

    def hear(gap):
        @pl.when((core == 1) & (z + gap <= last))
        def _():
            pl.semaphore_wait(up.at[gap - 2], 1)

        @pl.when((core == 1) & (z - gap >= 0))
        def _():
            pl.semaphore_wait(down.at[gap - 2], 1)

    rounds = [functools.partial(tell, 2)] if last >= 2 else []
    for gap in range(2, last + 1):
        rounds.append(functools.partial(hear, gap))
        if gap < last:
            rounds.append(functools.partial(tell, gap + 1))

    def column_entered():
        if column_known:
            return
        column_known.append(True)
        while rounds:
            rounds.pop(0)()

        @pl.when(core == 1)
        def _():
            signal(ready, {"dom": peer})

        @pl.when(core == 0)
        def _():
            pl.semaphore_wait(ready, 1)

    def forward(index):
        step, part, start, count, kind, _ = units[index]
        first[index].wait()
        got = scale_of(r1[step, :, head(index)])
        code = scale_code(jnp.maximum(tops[index, pl.ds(0, PAIR_ROWS)], TINY) + got)
        bound = scale_of(code)
        tops[index, pl.ds(0, PAIR_ROWS)] = bound
        q2[step, :, head(index)] = code[GROUP_ROWS:]
        if index == 0:
            tally = counts[:PAIR_ROWS] + from_code(r1[step, :, head(index, 1)])
            tallies[...] = tally
            q2[step, :, head(index, 1)] = to_code(tally)[GROUP_ROWS:]
        scale = got * (1.0 / LEVELS)
        factor = LEVELS / bound

        def body(span, unit):
            there = shifted(span, index)
            total = sums[step, pl.ds(0, PAIR_ROWS), span] + from_code(r1[step, :, there]) * wide(scale, unit)
            sums[step, pl.ds(0, PAIR_ROWS), span] = total
            q2[step, :, there] = to_code(total * wide(factor, unit))[GROUP_ROWS:]

        walk(start, count, CODE_TILES, body)
        other = far if kind == 0 else near
        second[index] = send(
            wire(q2, index, index == 0), wire(r2, index, index == 0),
            (s1.at[number(index)], g2.at[number(index)]), {"cls": other},
        )

    def settle(index):
        step, part, start, count, kind, _ = units[index]
        second[index].wait()
        if index == 0:
            column_entered()
            t3[...] = tallies[pl.ds(0, GROUP_ROWS)] + from_code(r2[step, :, head(index, 1)])
            for other in range(last):
                tally_copies.append(
                    send(t3, u3.at[other], (ts.at[other], tg.at[other]), {"dom": place(other) * 2 + core})
                )
        got = scale_of(r2[step, :, head(index)])
        scale = got * (1.0 / LEVELS)
        if step == last:

            def final_body(span, unit):
                there = shifted(span, index)
                value = sums[step, pl.ds(0, GROUP_ROWS), span] + from_code(r2[step, :, there]) * wide(scale, unit)
                mean_ref[:, span] = value * inverse[:, span]

            walk(start, count, CODE_TILES, final_body)
            return
        code = scale_code(tops[index, pl.ds(0, GROUP_ROWS)] + got)
        q3[step, :, head(index)] = code
        factor = LEVELS / scale_of(code)

        def body(span, unit):
            there = shifted(span, index)
            value = sums[step, pl.ds(0, GROUP_ROWS), span] + from_code(r2[step, :, there]) * wide(scale, unit)
            q3[step, :, there] = to_code(value * wide(factor, unit))

        walk(start, count, CODE_TILES, body)
        third[index] = send(
            wire(q3, index), wire(r3, index), (s1.at[number(index)], g3.at[number(index)]),
            {"dom": place(step) * 2 + core},
        )

    def gather(index):
        step, part, start, count, kind, _ = units[index]
        third[index].wait()
        scale = scale_of(r3[step, :, head(index)]) * (1.0 / LEVELS)

        def body(span, unit):
            sums[last, pl.ds(0, GROUP_ROWS), span] = sums[last, pl.ds(0, GROUP_ROWS), span] + from_code(
                r3[step, :, shifted(span, index)]
            ) * wide(scale, unit)

        walk(start, count, CODE_TILES, body)

    def tally_final():
        tally = t3[...]
        for step in range(last):
            tally_copies[step].wait()
            tally = tally + u3[step]
        high = tally.astype(jnp.bfloat16).astype(jnp.float32)
        tally = jnp.concatenate([high, tally - high], axis=0)[:, : 2 * slots].astype(jnp.bfloat16)

        def body(span, unit):
            weight = filled(table[last, :, span])
            total = dot(tally, stack2(weight * weight))
            total = total[:GROUP_ROWS] + total[GROUP_ROWS:]
            total_ref[:, span] = total
            inverse[:, span] = 1.0 / (total + 1.0)

        walk(0, tiles, SUM_TILES, body)

    for name, index in script:
        if name == "P":
            pick_weights(index)
        elif name in "CZ":
            compute(index)
            for _ in range(min(len(rounds), 2 if index else 1)):
                rounds.pop(0)()
        elif name == "F":
            forward(index)
        elif name == "S":
            settle(index)
        elif name == "G":
            gather(index)
        else:
            tally_final()
            sent = x_all.at[:, pl.ds(rows, rows)]
            pltpu.make_async_copy(sent, sent, pair_send).wait()


def finish(mean_ref, total_ref, avg_out, total_out, sem):
    copies = []
    for index in range(avg_out.shape[0]):
        copies.append(
            pltpu.make_async_copy(mean_ref.at[pl.ds(2 * index, 2)], avg_out.at[index], sem.at[2 * index])
        )
        copies.append(
            pltpu.make_async_copy(
                total_ref.at[pl.ds(2 * index, 1)], total_out.at[pl.ds(index, 1)], sem.at[2 * index + 1]
            )
        )
    for copy in copies:
        copy.start()
    for copy in copies:
        copy.wait()


def per_device(particles, labels, wedge_index, wedge_table):
    n_dom = lax.axis_size("dom")
    p_dev, _, voxels = particles.shape
    wedges = wedge_table.shape[0]
    shard = voxels // n_dom
    n_z = n_dom // 2
    rows = 2 * p_dev
    tiles = shard // LANES
    units, pairs, firsts = plan_units(n_z, tiles)
    order = plan_order(n_z, units, pairs, firsts)
    count = len(units)
    widest = max([units[k][3] for k in firsts], default=0) + 1
    parts = max(unit[1] for unit in units) + 1
    any_space = pl.BlockSpec(memory_space=pl.ANY)
    vmem = pl.BlockSpec(memory_space=pltpu.VMEM)
    dma = pltpu.SemaphoreType.DMA
    f32 = jnp.float32
    scratch = [
        pltpu.SMEM((p_dev,), jnp.int32),
        pltpu.SMEM((p_dev,), jnp.int32),
        pltpu.VMEM((3, rows, LANES), f32),
        pltpu.VMEM((3, rows, LANES), f32),
        pltpu.VMEM((n_z, 2 * rows, shard), jnp.bfloat16),
        pltpu.VMEM((n_z, wedges, shard), f32),
        pltpu.VMEM((n_z, 2 * rows, shard), f32),
        pltpu.VMEM((n_z, 4 * GROUP_ROWS, shard), f32),
        pltpu.VMEM((GROUP_ROWS, shard), f32),
        pltpu.VMEM((count, 4 * GROUP_ROWS, LANES), f32),
        pltpu.VMEM((PAIR_ROWS, LANES), f32),
    ]
    long = shard + parts * HEAD * LANES
    scratch += [pltpu.VMEM((max(len(firsts), 1), 4 * GROUP_ROWS, widest * LANES), jnp.int16)] * 2
    for height in (PAIR_ROWS, GROUP_ROWS, GROUP_ROWS):
        scratch += [pltpu.VMEM((n_z, height, long), jnp.int16)] * 2
    scratch += [pltpu.VMEM((GROUP_ROWS, LANES), f32), pltpu.VMEM((n_z, GROUP_ROWS, LANES), f32)]
    scratch += [dma((2,)), dma((n_z, 2)), dma((n_z,)), dma, dma((n_z, 2)), dma, dma]
    remote = len([unit for unit in units if unit[0] < n_z - 1 and not unit[5]])
    scratch += [dma((max(len(firsts), 1),))] * 2 + [dma((count - len(firsts),))] * 3 + [dma((remote,))]
    scratch += [dma((n_z - 1,))] * 2 + [pltpu.SemaphoreType.REGULAR]
    scratch += [pltpu.SemaphoreType.REGULAR((max(n_z - 2, 1),))] * 2
    mean, total = pl.pallas_call(
        functools.partial(kernel, n_z, shard, p_dev, wedges, units, order),
        out_shape=(
            pltpu.VMEM((GROUP_ROWS, shard), f32),
            pltpu.VMEM((GROUP_ROWS, shard), f32),
        ),
        in_specs=[any_space] * 4,
        out_specs=(vmem, vmem),
        scratch_shapes=scratch,
        compiler_params=pltpu.CompilerParams(
            collective_id=0, has_side_effects=True, vmem_limit_bytes=60 * 1024 * 1024
        ),
    )(labels.reshape(p_dev), wedge_index, particles, wedge_table)
    return pl.pallas_call(
        finish,
        out_shape=(
            jax.ShapeDtypeStruct((CLASSES_PER_GROUP, 2, shard), f32),
            jax.ShapeDtypeStruct((CLASSES_PER_GROUP, shard), f32),
        ),
        in_specs=[any_space, any_space],
        out_specs=(any_space, any_space),
        compiler_params=pltpu.CompilerParams(vmem_limit_bytes=4 * 1024 * 1024),
        scratch_shapes=[dma((2 * CLASSES_PER_GROUP,))],
    )(mean, total)


def solution(mesh):
    return jax.shard_map(
        per_device,
        mesh=mesh,
        in_specs=(P(("cls", "dom"), None, None), P(("cls", "dom"), None), P(("cls", "dom")), P()),
        out_specs=(P("cls", None, "dom"), P("cls", "dom")),
        check_vma=False,
    )
```

```python
import functools

import jax
import jax.numpy as jnp
from jax import lax
from jax.experimental import pallas as pl
from jax.experimental.pallas import tpu as pltpu
from jax.sharding import PartitionSpec as P

MESH = pl.DeviceIdType.MESH
LANES = 128
LEVELS = 32767.0
SCALE_STEPS = 128.0
TINY = 1e-30
HEAD = 2
CLASSES_PER_GROUP = 2
GROUP_ROWS = 2 * CLASSES_PER_GROUP
PAIR_ROWS = 2 * GROUP_ROWS
PICK_TILES = 108
SUM_TILES = 54
CODE_TILES = 54
AHEAD = 2
SETTLE_AFTER = 1
OWN_PAIRS = 2
EARLY_SHARE = 0.45


def divisor(number, cap):
    return max(size for size in range(1, cap + 1) if number % size == 0)


def padded(count):
    return -(-count // 16) * 16


def filled(value):
    extra = padded(value.shape[0]) - value.shape[0]
    if extra == 0:
        return value
    return jnp.concatenate([value, jnp.zeros((extra, value.shape[1]), value.dtype)], axis=0)


def dot(left, right):
    return jnp.dot(left, right, preferred_element_type=jnp.float32)


def stack2(value):
    high = value.astype(jnp.bfloat16)
    low = (value - high.astype(jnp.float32)).astype(jnp.bfloat16)
    return jnp.concatenate([high, low], axis=0)


def walk(start, tiles, cap, body):
    unit = divisor(tiles, cap)
    turns = tiles // unit
    if turns == 1:
        body(pl.ds(start, unit * LANES), unit)
        return

    @pl.loop(0, turns)
    def _(index):
        body(pl.ds(pl.multiple_of(start + index * (unit * LANES), LANES), unit * LANES), unit)


def wide(value, unit):
    return jnp.concatenate([value] * unit, axis=1) if unit > 1 else value


def to_code(value):
    return jnp.round(value).astype(jnp.int32).astype(jnp.int16)


def from_code(code):
    return code.astype(jnp.int32).astype(jnp.float32)


def scale_code(bound):
    return (jnp.ceil(jnp.log2(bound) * SCALE_STEPS) + 1.0).astype(jnp.int32).astype(jnp.int16)


def scale_of(code):
    return jnp.exp2(from_code(code) * (1.0 / SCALE_STEPS))


def plan_units(n_z, tiles):
    half = tiles // 2
    early = int(tiles * EARLY_SHARE / 2)
    units, pairs, firsts = [], [], []

    def add(step, pieces, early=False):
        base = sum(1 for unit in units if unit[0] == step)
        names = []
        for part, (start, count, kind) in enumerate(pieces):
            names.append(len(units))
            units.append((step, base + part, start * LANES, count, kind, early))
        return names

    for step in range(n_z):
        if step == n_z - 2 and early:
            firsts = add(step, ((0, early, 0), (half, early, 1)), True)
            pairs.append(add(step, ((early, half - early, 0), (half + early, tiles - half - early, 1))))
        elif step == n_z - 1 and OWN_PAIRS == 2 and half >= 2:
            cut = half // 2
            pairs.append(add(step, ((0, cut, 0), (half, cut, 1))))
            pairs.append(add(step, ((cut, half - cut, 0), (half + cut, tiles - half - cut, 1))))
        else:
            pairs.append(add(step, ((0, half, 0), (half, tiles - half, 1))))
    starts = [sorted(unit[2] for unit in units if unit[0] == step) for step in range(n_z)]
    units = [(unit[0], starts[unit[0]].index(unit[2]), *unit[2:]) for unit in units]
    return units, pairs, firsts


def plan_order(n_z, units, pairs, firsts):
    order, count = [], len(pairs)
    own = [k for k, unit in enumerate(units) if unit[0] == n_z - 1]
    ready = set()

    def weights(step):
        if step not in ready:
            ready.add(step)
            order.append(("P", step))

    def compute(j):
        if j < count:
            weights(units[pairs[j][0]][0])
            order.extend(("C", k) for k in pairs[j])

    compute(0)
    if firsts:
        weights(n_z - 2)
        order.extend(("Z", k) for k in firsts)
    for j in range(1, AHEAD):
        compute(j)
    remote = [k for k, unit in enumerate(units) if unit[0] < n_z - 1 and not unit[5]]
    for j in range(count):
        if j == count - 1:
            order.append(("T", 0))
        order.extend(("F", k) for k in pairs[j])
        compute(j + AHEAD)
        if j >= SETTLE_AFTER:
            order.extend(("S", k) for k in pairs[j - SETTLE_AFTER] if k not in own)
    late = [k for pair in pairs[count - SETTLE_AFTER :] for k in pair]
    order.extend(("S", k) for k in late if k not in own)
    order.extend(("G", k) for k in remote)
    order.extend(("S", k) for k in own)
    return order


def kernel(
    n_z, shard, p_dev, wedges, units, script,
    labels_ref, wedge_ref, x_ref, table_ref, mean_ref, total_ref,
    label_s, wedge_s, aux_own, aux_peer, x_all, table, weights, sums, inverse, tops, tallies,
    q0, r0, q1, r1, q2, r2, q3, r3, t3, u3,
    small_sem, load_sem, table_sem, pair_send, pair_recv, aux_send, aux_recv,
    s0, g0, s1, g1, g2, g3, ts, tg, ready, up, down,
):
    cls = lax.axis_index("cls")
    dom = lax.axis_index("dom")
    z = dom // 2
    core = lax.rem(dom, 2)
    peer = dom + 1 - 2 * core
    near = cls + 1 - 2 * lax.rem(cls, 2)
    far = cls + 2 - 4 * (cls // 2)
    both = near + 2 - 4 * (cls // 2)
    rows = 2 * p_dev
    tiles = shard // LANES
    last = n_z - 1
    slots = padded(wedges)
    offsets = sorted(range(1, n_z), key=lambda gap: -min(gap, n_z - gap)) + [0]

    def place(step):
        return lax.rem(z + offsets[step], n_z)

    small = [
        pltpu.make_async_copy(labels_ref, label_s, small_sem.at[0]),
        pltpu.make_async_copy(wedge_ref, wedge_s, small_sem.at[1]),
    ]
    for copy in small:
        copy.start()

    barrier = pltpu.get_barrier_semaphore()

    def signal(sem, who):
        pl.semaphore_signal(sem, inc=1, device_id=who, device_id_type=MESH)

    @pl.when(core == 1)
    def _():
        signal(barrier, {"dom": peer})

    loads, tables, pair = [], [], []

    def chunks(step, where):
        base = (place(step) * 2 + where) * shard
        cut = tiles // 2 * LANES if step == 0 else 0
        spans = [(0, cut), (cut, shard - cut)] if cut else [(0, shard)]
        return [
            (pl.ds(pl.multiple_of(base + begin, LANES), size), pl.ds(begin, size))
            for begin, size in spans
        ]

    def load_step(step):
        here = place(step) * 2 + core
        span = pl.ds(pl.multiple_of(here * shard, LANES), shard)
        copy = pltpu.make_async_copy(
            table_ref.at[:, span], table.at[step], table_sem.at[step]
        )
        copy.start()
        tables.append(copy)
        waits = []
        for part, (source, target) in enumerate(chunks(step, core)):
            for p in range(p_dev):
                pltpu.make_async_copy(
                    x_ref.at[p, :, source], x_all.at[step, pl.ds(2 * p, 2), target],
                    load_sem.at[step, part],
                ).start()
            block = x_all.at[step, pl.ds(0, rows), target]
            waits.append(pltpu.make_async_copy(block, block, load_sem.at[step, part]))
        loads.append(waits)

    def pair_step(step):
        waits = []
        for part, (source, target) in enumerate(chunks(step, 1 - core)):
            def pair_copy(source, target):
                return pltpu.make_async_remote_copy(
                    src_ref=source, dst_ref=target,
                    send_sem=pair_send, recv_sem=pair_recv.at[step, part],
                    device_id={"dom": peer}, device_id_type=MESH,
                )

            for p in range(p_dev):
                pair_copy(
                    x_ref.at[p, :, source], x_all.at[step, pl.ds(rows + 2 * p, 2), target]
                ).start()
            block = x_all.at[step, pl.ds(rows, rows), target]
            waits.append(pair_copy(block, block))
        pair.append(waits)

    for step in range(n_z):
        load_step(step)

    @pl.when(core == 0)
    def _():
        pl.semaphore_wait(barrier, 1)
        signal(ready, {"dom": peer})

    @pl.when(core == 1)
    def _():
        pl.semaphore_wait(ready, 1)
        signal(barrier, {"cls": near})
        signal(barrier, {"cls": far})

        @pl.when(z > 0)
        def _():
            signal(barrier, {"dom": dom - 2})

        @pl.when(z < last)
        def _():
            signal(barrier, {"dom": dom + 2})


    for copy in small:
        copy.wait()
    row = lax.broadcasted_iota(jnp.int32, (rows, LANES), 0)
    lane = lax.broadcasted_iota(jnp.int32, (rows, LANES), 1)
    out_row = lax.broadcasted_iota(jnp.int32, (4 * GROUP_ROWS, LANES), 0)
    out_lane = lax.broadcasted_iota(jnp.int32, (4 * GROUP_ROWS, LANES), 1)
    wedge_of = jnp.zeros((rows, LANES), jnp.int32)
    label_of = jnp.zeros_like(out_row)
    particle = (out_lane & (rows - 1)) // 2
    for p in range(p_dev):
        wedge_of = jnp.where(row // 2 == p, wedge_s[p], wedge_of)
        label_of = jnp.where(particle == p, label_s[p], label_of)
    column = jnp.where(lane >= slots, lane - slots, lane)
    aux_own[0] = ((wedge_of == column) & (lane < 2 * slots)).astype(jnp.float32)
    within = (out_row // 2) % CLASSES_PER_GROUP
    place_of = out_row // GROUP_ROWS
    for kind, order in enumerate(((cls, far, near, both), (cls, near, far, both))):
        target = jnp.zeros_like(out_row)
        for slot, group in enumerate(order):
            target = jnp.where(place_of == slot, CLASSES_PER_GROUP * group + within, target)
        aux_own[1 + kind] = (
            (target == label_of) & ((out_row & 1) == (out_lane & 1))
        ).astype(jnp.float32)

    aux_copy = pltpu.make_async_remote_copy(
        src_ref=aux_own, dst_ref=aux_peer, send_sem=aux_send, recv_sem=aux_recv,
        device_id={"dom": peer}, device_id_type=MESH,
    )
    aux_copy.start()
    for step in range(n_z):
        pair_step(step)
    aux_copy.wait()

    own_side = (out_lane & rows) == 0
    members = [
        jnp.where(own_side, aux_own[1 + kind], aux_peer[1 + kind])[:, : 4 * rows].astype(jnp.bfloat16)
        for kind in range(2)
    ]
    pick = jnp.concatenate([aux_own[0], aux_peer[0]], axis=0).astype(jnp.bfloat16)
    counts = dot(members[0][:, : 2 * rows], pick)
    pick = pick[:, : 2 * slots]

    def send(source, target, sems, who):
        copy = pltpu.make_async_remote_copy(
            src_ref=source, dst_ref=target, send_sem=sems[0], recv_sem=sems[1],
            device_id=who, device_id_type=MESH,
        )
        copy.start()
        return copy

    def pick_weights(step):
        tables[step].wait()

        def body(span, unit):
            weights[step, :, span] = dot(pick, stack2(filled(table[step, :, span])))

        walk(0, tiles, PICK_TILES, body)

    def wire(ref, index, tally=False):
        step, part, start, count, kind, _ = units[index]
        begin = start + part * (HEAD * LANES)
        return ref.at[step, :, pl.ds(begin, (count + 1 + tally) * LANES)]

    def head(index, extra=0):
        step, part, start, count, kind, _ = units[index]
        return pl.ds(start + part * (HEAD * LANES) + (count + extra) * LANES, LANES)

    def shifted(span, index):
        begin = span.start + units[index][1] * (HEAD * LANES)
        return pl.ds(begin if isinstance(begin, int) else pl.multiple_of(begin, LANES), span.size)

    zeroth, first, second, third, tally_copies = {}, {}, {}, {}, []
    column_known = []

    def pieces_of(index):
        step, part, start, count, kind, _ = units[index]
        if step != last:
            return [(start, count, None)]
        pieces, at, end = [], start, start + count * LANES
        for k, unit in enumerate(units):
            low, high = max(at, unit[2]), min(end, unit[2] + unit[3] * LANES)
            if unit[5] and low < high:
                if low > at:
                    pieces.append((at, (low - at) // LANES, None))
                pieces.append((low, (high - low) // LANES, k))
                at = high
        if at < end:
            pieces.append((at, (end - at) // LANES, None))
        return pieces

    def number(index):
        return index - len([k for k in range(index) if units[k][5]])

    def early_slot(index):
        slot = [k for k, unit in enumerate(units) if unit[5]].index(index)
        return slot, (units[index][3] + 1) * LANES

    def early_wire(ref, index):
        slot, size = early_slot(index)
        return ref.at[slot, :, pl.ds(0, size)]

    loaded, landed = set(), set()

    def compute(index):
        step, part, start, count, kind, early = units[index]
        groups = len(loads[step])
        for group in range(1 if groups > 1 and start + count * LANES <= tiles // 2 * LANES else groups):
            if (step, group) not in loaded:
                loaded.add((step, group))
                loads[step][group].wait()
                pair[step][group].wait_recv()
        member = members[kind]
        tops[index] = jnp.zeros((4 * GROUP_ROWS, LANES), jnp.float32)
        for begin, length, source in pieces_of(index):
            scale = None
            if source is not None:
                slot = early_slot(source)[0]
                if source not in landed:
                    landed.add(source)
                    zeroth[source].wait()
                origin = units[source][2]
                scale = scale_of(r0[slot, :, pl.ds(units[source][3] * LANES, LANES)]) * (1.0 / LEVELS)

            def body(span, unit):
                product = weights[step, :, span] * x_all[step, :, span].astype(jnp.float32)
                total = dot(member, stack2(product))
                if scale is not None:
                    at = span.start - origin
                    there = pl.ds(at if isinstance(at, int) else pl.multiple_of(at, LANES), span.size)
                    total = total + from_code(r0[slot, :, there]) * wide(scale, unit)
                sums[step, :, span] = total
                size = jnp.abs(total)
                parts = [size[:, k * LANES : (k + 1) * LANES] for k in range(unit)]
                while len(parts) > 1:
                    parts = [
                        jnp.maximum(*parts[k : k + 2]) if k + 1 < len(parts) else parts[k]
                        for k in range(0, len(parts), 2)
                    ]
                tops[index] = jnp.maximum(tops[index], parts[0])

            walk(begin, length, SUM_TILES, body)
        span = pl.ds(start, count * LANES)
        if early:
            slot, size = early_slot(index)
            code = scale_code(jnp.maximum(tops[index], TINY))
            q0[slot, :, pl.ds(count * LANES, LANES)] = code
            factor = LEVELS / scale_of(code)

            def early_body(span, unit):
                at = span.start - start
                there = pl.ds(at if isinstance(at, int) else pl.multiple_of(at, LANES), span.size)
                q0[slot, :, there] = to_code(sums[step, :, span] * wide(factor, unit))

            walk(start, count, CODE_TILES, early_body)
            column_entered()
            zeroth[index] = send(
                early_wire(q0, index), early_wire(r0, index), (s0.at[slot], g0.at[slot]),
                {"dom": place(step) * 2 + core},
            )
            return
        code = scale_code(jnp.maximum(tops[index, pl.ds(PAIR_ROWS, PAIR_ROWS)], TINY))
        q1[step, :, head(index)] = code
        if index == 0:
            q1[step, :, head(index, 1)] = to_code(counts[PAIR_ROWS:])
        factor = LEVELS / scale_of(code)

        def code_body(span, unit):
            q1[step, :, shifted(span, index)] = to_code(
                sums[step, pl.ds(PAIR_ROWS, PAIR_ROWS), span] * wide(factor, unit)
            )

        walk(start, count, CODE_TILES, code_body)
        if index == 0:
            all_entered()
        partner = near if kind == 0 else far
        first[index] = send(
            wire(q1, index, index == 0), wire(r1, index, index == 0),
            (s1.at[number(index)], g1.at[number(index)]), {"cls": partner},
        )

    def all_entered():
        @pl.when(core == 1)
        def _():
            pl.semaphore_wait(barrier, 2 + jnp.minimum(z, 1) + jnp.minimum(last - z, 1))
            signal(ready, {"dom": peer})

        @pl.when(core == 0)
        def _():
            pl.semaphore_wait(ready, 1)

    def tell(gap):
        @pl.when((core == 1) & (z > 0) & (z + gap - 1 <= last))
        def _():
            signal(up.at[gap - 2], {"dom": dom - 2})

        @pl.when((core == 1) & (z < last) & (z - gap + 1 >= 0))
        def _():
            signal(down.at[gap - 2], {"dom": dom + 2})

    def hear(gap):
        @pl.when((core == 1) & (z + gap <= last))
        def _():
            pl.semaphore_wait(up.at[gap - 2], 1)

        @pl.when((core == 1) & (z - gap >= 0))
        def _():
            pl.semaphore_wait(down.at[gap - 2], 1)

    rounds = [functools.partial(tell, 2)] if last >= 2 else []
    for gap in range(2, last + 1):
        rounds.append(functools.partial(hear, gap))
        if gap < last:
            rounds.append(functools.partial(tell, gap + 1))

    def column_entered():
        if column_known:
            return
        column_known.append(True)
        while rounds:
            rounds.pop(0)()

        @pl.when(core == 1)
        def _():
            signal(ready, {"dom": peer})

        @pl.when(core == 0)
        def _():
            pl.semaphore_wait(ready, 1)

    def forward(index):
        step, part, start, count, kind, _ = units[index]
        first[index].wait()
        got = scale_of(r1[step, :, head(index)])
        code = scale_code(jnp.maximum(tops[index, pl.ds(0, PAIR_ROWS)], TINY) + got)
        bound = scale_of(code)
        tops[index, pl.ds(0, PAIR_ROWS)] = bound
        q2[step, :, head(index)] = code[GROUP_ROWS:]
        if index == 0:
            tally = counts[:PAIR_ROWS] + from_code(r1[step, :, head(index, 1)])
            tallies[...] = tally
            q2[step, :, head(index, 1)] = to_code(tally)[GROUP_ROWS:]
        scale = got * (1.0 / LEVELS)
        factor = LEVELS / bound

        def body(span, unit):
            there = shifted(span, index)
            total = sums[step, pl.ds(0, PAIR_ROWS), span] + from_code(r1[step, :, there]) * wide(scale, unit)
            sums[step, pl.ds(0, PAIR_ROWS), span] = total
            q2[step, :, there] = to_code(total * wide(factor, unit))[GROUP_ROWS:]

        walk(start, count, CODE_TILES, body)
        other = far if kind == 0 else near
        second[index] = send(
            wire(q2, index, index == 0), wire(r2, index, index == 0),
            (s1.at[number(index)], g2.at[number(index)]), {"cls": other},
        )

    def settle(index):
        step, part, start, count, kind, _ = units[index]
        second[index].wait()
        if index == 0:
            column_entered()
            t3[...] = tallies[pl.ds(0, GROUP_ROWS)] + from_code(r2[step, :, head(index, 1)])
            for other in range(last):
                tally_copies.append(
                    send(t3, u3.at[other], (ts.at[other], tg.at[other]), {"dom": place(other) * 2 + core})
                )
        got = scale_of(r2[step, :, head(index)])
        scale = got * (1.0 / LEVELS)
        if step == last:

            def final_body(span, unit):
                there = shifted(span, index)
                value = sums[step, pl.ds(0, GROUP_ROWS), span] + from_code(r2[step, :, there]) * wide(scale, unit)
                mean_ref[:, span] = value * inverse[:, span]

            walk(start, count, CODE_TILES, final_body)
            return
        code = scale_code(tops[index, pl.ds(0, GROUP_ROWS)] + got)
        q3[step, :, head(index)] = code
        factor = LEVELS / scale_of(code)

        def body(span, unit):
            there = shifted(span, index)
            value = sums[step, pl.ds(0, GROUP_ROWS), span] + from_code(r2[step, :, there]) * wide(scale, unit)
            q3[step, :, there] = to_code(value * wide(factor, unit))

        walk(start, count, CODE_TILES, body)
        third[index] = send(
            wire(q3, index), wire(r3, index), (s1.at[number(index)], g3.at[number(index)]),
            {"dom": place(step) * 2 + core},
        )

    def gather(index):
        step, part, start, count, kind, _ = units[index]
        third[index].wait()
        scale = scale_of(r3[step, :, head(index)]) * (1.0 / LEVELS)

        def body(span, unit):
            sums[last, pl.ds(0, GROUP_ROWS), span] = sums[last, pl.ds(0, GROUP_ROWS), span] + from_code(
                r3[step, :, shifted(span, index)]
            ) * wide(scale, unit)

        walk(start, count, CODE_TILES, body)

    def tally_final():
        tally = t3[...]
        for step in range(last):
            tally_copies[step].wait()
            tally = tally + u3[step]
        high = tally.astype(jnp.bfloat16).astype(jnp.float32)
        tally = jnp.concatenate([high, tally - high], axis=0)[:, : 2 * slots].astype(jnp.bfloat16)

        def body(span, unit):
            weight = filled(table[last, :, span])
            total = dot(tally, stack2(weight * weight))
            total = total[:GROUP_ROWS] + total[GROUP_ROWS:]
            total_ref[:, span] = total
            inverse[:, span] = 1.0 / (total + 1.0)

        walk(0, tiles, SUM_TILES, body)

    for name, index in script:
        if name == "P":
            pick_weights(index)
        elif name in "CZ":
            compute(index)
            for _ in range(min(len(rounds), 2 if index else 1)):
                rounds.pop(0)()
        elif name == "F":
            forward(index)
        elif name == "S":
            settle(index)
        elif name == "G":
            gather(index)
        else:
            tally_final()
            sent = x_all.at[:, pl.ds(rows, rows)]
            pltpu.make_async_copy(sent, sent, pair_send).wait()


def finish(mean_ref, total_ref, avg_out, total_out, sem):
    copies = []
    for index in range(avg_out.shape[0]):
        copies.append(
            pltpu.make_async_copy(mean_ref.at[pl.ds(2 * index, 2)], avg_out.at[index], sem.at[2 * index])
        )
        copies.append(
            pltpu.make_async_copy(
                total_ref.at[pl.ds(2 * index, 1)], total_out.at[pl.ds(index, 1)], sem.at[2 * index + 1]
            )
        )
    for copy in copies:
        copy.start()
    for copy in copies:
        copy.wait()


def per_device(particles, labels, wedge_index, wedge_table):
    n_dom = lax.axis_size("dom")
    p_dev, _, voxels = particles.shape
    wedges = wedge_table.shape[0]
    shard = voxels // n_dom
    n_z = n_dom // 2
    rows = 2 * p_dev
    tiles = shard // LANES
    units, pairs, firsts = plan_units(n_z, tiles)
    order = plan_order(n_z, units, pairs, firsts)
    count = len(units)
    widest = max([units[k][3] for k in firsts], default=0) + 1
    parts = max(unit[1] for unit in units) + 1
    any_space = pl.BlockSpec(memory_space=pl.ANY)
    vmem = pl.BlockSpec(memory_space=pltpu.VMEM)
    dma = pltpu.SemaphoreType.DMA
    f32 = jnp.float32
    scratch = [
        pltpu.SMEM((p_dev,), jnp.int32),
        pltpu.SMEM((p_dev,), jnp.int32),
        pltpu.VMEM((3, rows, LANES), f32),
        pltpu.VMEM((3, rows, LANES), f32),
        pltpu.VMEM((n_z, 2 * rows, shard), jnp.bfloat16),
        pltpu.VMEM((n_z, wedges, shard), f32),
        pltpu.VMEM((n_z, 2 * rows, shard), f32),
        pltpu.VMEM((n_z, 4 * GROUP_ROWS, shard), f32),
        pltpu.VMEM((GROUP_ROWS, shard), f32),
        pltpu.VMEM((count, 4 * GROUP_ROWS, LANES), f32),
        pltpu.VMEM((PAIR_ROWS, LANES), f32),
    ]
    long = shard + parts * HEAD * LANES
    scratch += [pltpu.VMEM((max(len(firsts), 1), 4 * GROUP_ROWS, widest * LANES), jnp.int16)] * 2
    for height in (PAIR_ROWS, GROUP_ROWS, GROUP_ROWS):
        scratch += [pltpu.VMEM((n_z, height, long), jnp.int16)] * 2
    scratch += [pltpu.VMEM((GROUP_ROWS, LANES), f32), pltpu.VMEM((n_z, GROUP_ROWS, LANES), f32)]
    scratch += [dma((2,)), dma((n_z, 2)), dma((n_z,)), dma, dma((n_z, 2)), dma, dma]
    remote = len([unit for unit in units if unit[0] < n_z - 1 and not unit[5]])
    scratch += [dma((max(len(firsts), 1),))] * 2 + [dma((count - len(firsts),))] * 3 + [dma((remote,))]
    scratch += [dma((n_z - 1,))] * 2 + [pltpu.SemaphoreType.REGULAR]
    scratch += [pltpu.SemaphoreType.REGULAR((max(n_z - 2, 1),))] * 2
    mean, total = pl.pallas_call(
        functools.partial(kernel, n_z, shard, p_dev, wedges, units, order),
        out_shape=(
            pltpu.VMEM((GROUP_ROWS, shard), f32),
            pltpu.VMEM((GROUP_ROWS, shard), f32),
        ),
        in_specs=[any_space] * 4,
        out_specs=(vmem, vmem),
        scratch_shapes=scratch,
        compiler_params=pltpu.CompilerParams(
            collective_id=0, has_side_effects=True, vmem_limit_bytes=60 * 1024 * 1024
        ),
    )(labels.reshape(p_dev), wedge_index, particles, wedge_table)
    return pl.pallas_call(
        finish,
        out_shape=(
            jax.ShapeDtypeStruct((CLASSES_PER_GROUP, 2, shard), f32),
            jax.ShapeDtypeStruct((CLASSES_PER_GROUP, shard), f32),
        ),
        in_specs=[any_space, any_space],
        out_specs=(any_space, any_space),
        compiler_params=pltpu.CompilerParams(vmem_limit_bytes=4 * 1024 * 1024),
        scratch_shapes=[dma((2 * CLASSES_PER_GROUP,))],
    )(mean, total)


def solution(mesh):
    return jax.shard_map(
        per_device,
        mesh=mesh,
        in_specs=(P(("cls", "dom"), None, None), P(("cls", "dom"), None), P(("cls", "dom")), P()),
        out_specs=(P("cls", None, "dom"), P("cls", "dom")),
        check_vma=False,
    )
```
